32 devices in a mesh: sub: 8 (over z, y), grp: 4 (over x, core).
Axes of the slice: x: 2, y: 2, z: 4, core: 2. Of those that a mesh axis runs over, the one named last changes fastest.
Arguments:
- rr_inverse: float32 [64, 512, 512], P(('sub', 'grp')), may hold values from -4 to 4, as said below
- corner_modes: float32 [64, 64, 512], P(('sub', 'grp')), may hold values from -0.5 to 0.5
- coarse_inverse: float32 [2048, 2048], P(('sub', 'grp')), may hold values from -1 to 1, as said below
- inertia: float32 [64, 512], P(('sub', 'grp')), may hold values from 0.5 to 2
- disp_now: float32 [8, 64, 512], P(None, ('sub', 'grp')), may hold values from -4 to 4
- vel_now: float32 [8, 64, 512], P(None, ('sub', 'grp')), may hold values from -4 to 4
- acc_now: float32 [8, 64, 512], P(None, ('sub', 'grp')), may hold values from -8 to 8
- load_next: float32 [8, 64, 512], P(None, ('sub', 'grp')), may hold values from -10 to 10
- basis_rows: float32 [32768, 256], P(('sub', 'grp')), may hold values from -0.03125 to 0.03125
- piece_owner: int32 [32], replicated, may hold values from 0 to 31, each once
Outputs:
- disp_new: float32 [8, 64, 512], P(None, ('sub', 'grp'))
- vel_new: float32 [8, 64, 512], P(None, ('sub', 'grp'))
- projection: float32 [256, 8], replicated
- r_factor: float32 [8, 8], replicated
- new_columns: float32 [8, 32768], P(None, ('sub', 'grp'))
The draws below stay inside these ranges and needn't reach their ends.
Inputs may be any that keep to these rules, and one draw needn't show every extreme that they name: piece_owner is a permutation. `rr_inverse`: each of the 64 blocks is symmetric positive definite. `coarse_inverse`: symmetric positive definite.
All inputs are finite; a program needn't handle non-finite values.
Results may differ from the reference program's by a relative error of at most 0.00018.
Values sent between devices are 32-bit elements; how exact they have to be, the bound alone decides.
A program may use at most 64 MiB of HBM per device.

```python
import math
import jax
import jax.numpy as jnp
from jax import lax

NR = 512
NC = 32
RANK = 256
NCASE = 8
ITERS = 2
NI = 128
SUBDOMAINS = 64
NCG = 2048
NROWS = 32768
PIECES = 32


def coupled_block(key, order, floor_value, ceiling_value, shared):
    key_noise, key_diag = jax.random.split(key)
    noise = jax.random.uniform(key_noise, (order, order), jnp.float32, -1.0, 1.0)
    upper = jnp.triu(noise, 1)
    coupling = (upper + upper.T) * (0.3 * math.sqrt(3.0) / math.sqrt(order))
    logs = jax.random.uniform(key_diag, (order,), jnp.float32, math.log(floor_value), math.log(ceiling_value))
    roots = jnp.exp(0.5 * logs)
    middle = jnp.eye(order, dtype=jnp.float32) + coupling + shared / order
    return roots[:, None] * middle * roots[None, :]


def draw_rr_inverse(key, part):
    subkeys = jax.random.split(key, SUBDOMAINS)
    return lax.map(lambda single: coupled_block(single, NR, 0.05, 2.0, 0.0), subkeys)


def draw_coarse_inverse(key, part):
    return coupled_block(key, NCG, 0.1, 0.5, 0.3)


def draw_load_next(key, part):
    key_base, key_rows = jax.random.split(key, 2)
    position = jnp.arange(SUBDOMAINS, dtype=jnp.float32) / max(SUBDOMAINS - 1, 1)
    row_scale = 10.0 ** jax.random.uniform(key_rows, (1, SUBDOMAINS, NR), jnp.float32)
    base = jax.random.truncated_normal(key_base, -4.0, 4.0, (NCASE, SUBDOMAINS, NR), jnp.float32)
    ramp = 3.0 ** position
    return 0.04 * base * ramp[None, :, None] * row_scale


def shard_levels(rng, dims, cuts, low, largest):
    level, own = 1.0, jax.random.fold_in(rng, 6)
    for axis_at, blocks in cuts:
        draws = jnp.exp(jax.random.uniform(jax.random.fold_in(own, axis_at), (blocks,), jnp.float32, low / len(cuts), largest / len(cuts)))
        level = level * jnp.repeat(draws, dims[axis_at] // blocks).reshape([-1 if axis == axis_at else 1 for axis in range(len(dims))])
    return level


def gaussian(stream_key, dims, scale, most, shards=(), kind=jnp.bfloat16):
    values = jax.random.normal(stream_key, dims, jnp.float32) * scale
    if len(shards) > 0:
        values = shard_levels(stream_key, dims, shards, -0.22, 0.18) * values
    return jnp.clip(values, min=-most, max=most).astype(kind)


def setup_inputs(seed: int = 0) -> dict:
    key_of = jax.random.split(jax.random.key(seed), 11)
    return {
        "rr_inverse": draw_rr_inverse(jax.random.fold_in(key_of[10], 71), 0),
        "corner_modes": gaussian(key_of[1], (SUBDOMAINS, 2 * NC, NR), (NR // 4) ** -0.5, 0.5, ((0, 32),), jnp.float32),
        "coarse_inverse": draw_coarse_inverse(jax.random.fold_in(key_of[10], 71), 0),
        "inertia": jnp.clip(jnp.exp(math.log(2.0) - 1.3862944 * jax.random.uniform(key_of[3], (SUBDOMAINS, NR), jnp.float32) ** shard_levels(key_of[3], (SUBDOMAINS, NR), ((0, 32),), -0.2, 0.2)), 0.5, 2.0),
        "disp_now": gaussian(key_of[4], (NCASE, SUBDOMAINS, NR), 1.0, 4.0, ((1, 32),), jnp.float32),
        "vel_now": gaussian(key_of[5], (NCASE, SUBDOMAINS, NR), 1.0, 4.0, ((1, 32),), jnp.float32),
        "acc_now": gaussian(key_of[6], (NCASE, SUBDOMAINS, NR), 2.0, 8.0, ((1, 32),), jnp.float32),
        "load_next": draw_load_next(jax.random.fold_in(key_of[10], 71), 0),
        "basis_rows": gaussian(key_of[8], (NROWS, RANK), NROWS ** -0.5, 0.03125, ((0, 32),), jnp.float32),
        "piece_owner": jax.random.permutation(key_of[9], PIECES).astype(jnp.int32),
    }


highest = lax.Precision.HIGHEST
time_step = 0.5
newmark_beta = 0.25
newmark_gamma = 0.5

def green_apply(rr_inverse, corner_modes, coarse_inverse, field):

    def products(operands):
        return jnp.dot(operands[0], operands[1], precision=highest)
    local_part = lax.map(products, (rr_inverse, jnp.transpose(field, (1, 2, 0))))
    local_part = jnp.transpose(local_part, (2, 0, 1))
    corner_terms = jnp.einsum('kmb,ckb->ckm', corner_modes, field, precision=highest)
    assembled = corner_terms[:, :, NC:] + jnp.roll(corner_terms[:, :, :NC], -1, axis=1)
    coarse_rhs = assembled.reshape(NCASE, NCG)
    coarse_sol = lax.dot_general(coarse_rhs, coarse_inverse, (((1,), (1,)), ((), ())), precision=highest)
    coarse_sol = coarse_sol.reshape(NCASE, SUBDOMAINS, NC)
    coarse_values = jnp.concatenate([jnp.roll(coarse_sol, 1, axis=1), coarse_sol], axis=2)
    return local_part + jnp.einsum('kmb,ckm->ckb', corner_modes, coarse_values, precision=highest)

def interface_jump(field):
    return field[:, :, NR - NI:] - jnp.roll(field[:, :, :NI], -1, axis=1)

def spread(values):
    middle = jnp.zeros((NCASE, SUBDOMAINS, NR - 2 * NI), jnp.float32)
    return jnp.concatenate([-jnp.roll(values, 1, axis=1), middle, values], axis=2)

def reference(rr_inverse, corner_modes, coarse_inverse, inertia, disp_now, vel_now, acc_now, load_next, basis_rows, piece_owner):
    right_side = load_next + inertia[None] * (disp_now + time_step * vel_now + (0.5 - newmark_beta) * time_step * time_step * acc_now)
    green_rhs = green_apply(rr_inverse, corner_modes, coarse_inverse, right_side)
    residual = interface_jump(green_rhs)
    multipliers = jnp.zeros_like(residual)
    direction = residual
    norm_now = lax.optimization_barrier(jnp.sum(residual * residual, axis=(1, 2)))
    for iteration in range(ITERS):
        image = interface_jump(green_apply(rr_inverse, corner_modes, coarse_inverse, spread(direction)))
        curvature = lax.optimization_barrier(jnp.sum(direction * image, axis=(1, 2)))
        alpha = (norm_now / curvature)[:, None, None]
        multipliers = multipliers + alpha * direction
        residual = residual - alpha * image
        norm_next = lax.optimization_barrier(jnp.sum(residual * residual, axis=(1, 2)))
        direction = residual + (norm_next / norm_now)[:, None, None] * direction
        norm_now = norm_next
    disp_new = green_apply(rr_inverse, corner_modes, coarse_inverse, right_side - spread(multipliers))
    accel_new = (disp_new - disp_now) / (newmark_beta * time_step * time_step) - vel_now / (newmark_beta * time_step) - (0.5 / newmark_beta - 1.0) * acc_now
    vel_new = vel_now + time_step * ((1.0 - newmark_gamma) * acc_now + newmark_gamma * accel_new)
    inverse = jnp.zeros((PIECES,), jnp.int32).at[piece_owner].set(jnp.arange(PIECES, dtype=jnp.int32))
    piece_rows = NR // PIECES
    snapshots = disp_new.reshape(NCASE, SUBDOMAINS, PIECES, piece_rows)[:, :, inverse, :]
    snapshots = jnp.transpose(snapshots, (0, 2, 1, 3)).reshape(NCASE, NROWS)
    projection = lax.dot_general(basis_rows, snapshots, (((0,), (1,)), ((), ())), precision=highest)
    remainder = snapshots - lax.dot_general(projection, basis_rows, (((0,), (1,)), ((), ())), precision=highest)
    gram = lax.dot_general(remainder, remainder, (((1,), (1,)), ((), ())), precision=highest)
    lower = jnp.linalg.cholesky(gram)
    scale_rows = math.sqrt(NROWS)
    new_columns = jax.scipy.linalg.solve_triangular(lower, remainder, lower=True) * scale_rows
    r_factor = lower.T / scale_rows
    return (disp_new, vel_new, projection, r_factor, new_columns)
```

```python
import functools
import math

import jax
import jax.numpy as jnp
from jax import lax
from jax.experimental import pallas as pl
from jax.experimental.pallas import tpu as pltpu
from jax.sharding import PartitionSpec as P

NC = 32
NI = 128
LANES = 128

time_step = 0.5
newmark_beta = 0.25
newmark_gamma = 0.5

MESH = pl.DeviceIdType.MESH


def nn(a, b):
    return lax.dot_general(
        a, b, (((1,), (0,)), ((), ())), precision=lax.Precision.HIGHEST, preferred_element_type=jnp.float32
    )


def nt(a, b):
    return lax.dot_general(
        a, b, (((1,), (1,)), ((), ())), precision=lax.Precision.HIGHEST, preferred_element_type=jnp.float32
    )


def split(x):
    first = x.astype(jnp.bfloat16)
    rest = x - first.astype(jnp.float32)
    second = rest.astype(jnp.bfloat16)
    return first, second, (rest - second.astype(jnp.float32)).astype(jnp.bfloat16)


def keep_split(parts, matrix):
    for at, part in enumerate(split(matrix)):
        parts[at] = part


def split_dot(x, parts, contracted):
    first, second, third = split(x)
    stacked = jnp.concatenate([first, second, third, jnp.zeros_like(first)], axis=0)
    rows = x.shape[0]

    def product(a, b):
        return lax.dot_general(a, b, (((1,), (contracted,)), ((), ())), preferred_element_type=jnp.float32)

    large = product(stacked, parts[0])
    middle = product(stacked[: 2 * rows], parts[1])
    small = product(stacked[: 2 * rows], parts[2])
    correction = large[2 * rows : 3 * rows] + middle[rows : 2 * rows] + small[:rows]
    return large[:rows] + (large[rows : 2 * rows] + middle[:rows] + correction)


def hand_over(*refs):
    half = len(refs) // 2
    for source, target in zip(refs[:half], refs[half:]):
        target[...] = source[...]


def kernel(
    n,
    groups,
    inner,
    owner_hbm,
    rr_hbm,
    modes_hbm,
    coarse_hbm,
    basis_hbm,
    inertia_hbm,
    disp_hbm,
    vel_hbm,
    acc_hbm,
    load_hbm,
    disp_out,
    vel_out,
    proj_out,
    r_out,
    cols_out,
    owner,
    inverse,
    inertia,
    disp_now,
    vel_now,
    acc_now,
    load_next,
    coarse_parts,
    forward_parts,
    backward_parts,
    basis_parts,
    rr,
    modes,
    coarse,
    basis,
    modes_next,
    modes_prev,
    corner,
    forward,
    backward,
    gathered,
    edge,
    edge_out,
    norms,
    pieces,
    outgoing,
    incoming,
    proj_parts,
    proj_sums,
    gram_parts,
    green,
    local_sem,
    const_send,
    const_recv,
    wide_send,
    wide_recv,
    edge_send,
    edge_recv,
):
    sub_count, unknowns = rr.shape[0], rr.shape[1]
    rows = sub_count * NC
    me = lax.axis_index("sub") * groups + lax.axis_index("grp")
    following = lax.rem(me + 1, n)
    earlier = lax.rem(me + n - 1, n)
    odd = lax.rem(me, 2) == 1
    partner = jnp.where(odd, earlier, following)
    outward = jnp.where(odd, following, earlier)

    def device(rank):
        return (rank // groups, lax.rem(rank, groups))

    plane, outer = me // inner, n // inner
    seat = lax.rem(me, inner)
    seats = [lax.rem(2 * inner - 1 - seat + i, inner) for i in range(inner)]
    mirrored = 2 * plane > outer - 1
    depth = jnp.where(mirrored, outer - 1 - plane, plane)
    lead = outer - 1 - 2 * depth

    def others(body):
        def step(i, carry):
            beyond = i - lead
            turn = jnp.where(lax.rem(beyond, 2) == 0, 2 * depth - beyond // 2, beyond // 2)
            at = jnp.where(i < lead, outer - 1 - i, turn)
            at = jnp.where(mirrored, outer - 1 - at, at)
            for there in seats:
                body(at * inner + there)
            return carry

        lax.fori_loop(0, outer - 1, step, 0)
        for i in range(1, inner):
            body(plane * inner + lax.rem(seat + i, inner))

    def remote(src, dst, send, recv, rank):
        return pltpu.make_async_remote_copy(
            src_ref=src, dst_ref=dst, send_sem=send, recv_sem=recv, device_id=device(rank), device_id_type=MESH
        )

    barrier = pltpu.get_barrier_semaphore()
    others(lambda rank: pl.semaphore_signal(barrier, inc=1, device_id=device(rank), device_id_type=MESH))

    load_rr = pltpu.make_async_copy(rr_hbm, rr, local_sem.at[0])
    load_modes = pltpu.make_async_copy(modes_hbm, modes, local_sem.at[1])
    load_coarse = pltpu.make_async_copy(coarse_hbm, coarse.at[pl.ds(0, rows)], local_sem.at[2])
    load_basis = pltpu.make_async_copy(basis_hbm, basis, local_sem.at[3])
    fields_in = [
        pltpu.make_async_copy(source, target, local_sem.at[4 + at])
        for at, (source, target) in enumerate(
            (
                (inertia_hbm, inertia),
                (disp_hbm, disp_now),
                (vel_hbm, vel_now),
                (acc_hbm, acc_now),
                (load_hbm, load_next),
            )
        )
    ]
    load_owner = pltpu.make_async_copy(owner_hbm, owner, local_sem.at[9])
    load_modes.start()
    for copy in fields_in:
        copy.start()
    load_owner.start()
    load_coarse.start()
    load_rr.start()
    load_basis.start()

    lane = lax.broadcasted_iota(jnp.int32, (8, LANES), 1)
    sublane = lax.broadcasted_iota(jnp.int32, (8, LANES), 0)

    def right_side(k):
        return load_next[:, k, :] + inertia[k : k + 1, :] * (
            disp_now[:, k, :]
            + time_step * vel_now[:, k, :]
            + (0.5 - newmark_beta) * time_step * time_step * acc_now[:, k, :]
        )

    for copy in fields_in:
        copy.wait()
    sides = [right_side(k) for k in range(sub_count)]

    corner[...] = jnp.zeros_like(corner)
    load_modes.wait()
    corner[0:NC, 0:unknowns] = modes[0, NC:, :]
    corner[0:NC, unknowns:] = modes[1, :NC, :]
    corner[NC : 2 * NC, unknowns:] = modes[1, NC:, :]
    corner[3 * NC :, 0:unknowns] = modes[0, :NC, :]

    def placed(tile):
        return jnp.where(odd, pltpu.roll(tile, 64, 1), tile)

    def broadcast(buffer, at, sem):
        def send(rank):
            remote(buffer.at[at, me], buffer.at[at, me], wide_send.at[sem], wide_recv.at[sem], rank).start()

        others(send)

    def all_but_one(buffer, at, sem):
        return pltpu.make_async_copy(buffer.at[at, pl.ds(0, n - 1)], buffer.at[at, pl.ds(0, n - 1)], sem)

    gathered[0, me] = placed(nt(jnp.concatenate(sides, axis=1), corner[...]))

    pl.semaphore_wait(barrier, n - 1)
    broadcast(gathered, 0, 0)

    load_coarse.wait()
    halos = [
        remote(
            coarse.at[pl.ds(NC, NC)], coarse.at[pl.ds(3 * NC, NC)], const_send.at[0], const_recv.at[0], following
        ),
        remote(modes.at[1, :, pl.ds(unknowns - NI, NI)], modes_prev, const_send.at[1], const_recv.at[1], following),
        remote(modes.at[0, :, pl.ds(0, NI)], modes_next, const_send.at[2], const_recv.at[2], earlier),
        remote(coarse.at[pl.ds(0, NC)], coarse.at[pl.ds(2 * NC, NC)], const_send.at[3], const_recv.at[3], partner),
    ]
    for copy in halos:
        copy.start()

    load_rr.wait()
    local = [nn(sides[k], rr[k]) for k in range(sub_count)]
    def facing_edge(first, last, at):
        edge_out[at] = jnp.where(odd, first, last)
        copy = remote(edge_out.at[at], edge.at[at], edge_send.at[at], edge_recv.at[at], partner)
        copy.start()
        edges.append(copy)
        return copy

    edges = []
    met = facing_edge(local[0][:, :NI], local[1][:, unknowns - NI :], 0)

    load_owner.wait()

    def find(t, carry):
        at = jnp.int32(0)
        for p in range(n):
            at = jnp.where(owner[p] == t, p, at)
        inverse[t] = at
        return carry

    lax.fori_loop(0, n, find, 0)
    for copy in halos:
        copy.wait_recv()
    first0, last0 = modes[0, :, :NI], modes[0, :, unknowns - NI :]
    first1, last1 = modes[1, :, :NI], modes[1, :, unknowns - NI :]
    before, after = modes_prev[...], modes_next[...]
    forward[...] = jnp.zeros_like(forward)
    forward[0:NC, 0:NI] = -first0[NC:]
    forward[0:NC, NI : 2 * NI] = last0[NC:] - first1[:NC]
    forward[0:NC, 2 * NI :] = last1[:NC]
    forward[NC : 2 * NC, NI : 2 * NI] = -first1[NC:]
    forward[NC : 2 * NC, 2 * NI :] = last1[NC:] - jnp.where(odd, 0.0, after[:NC])
    forward[2 * NC : 3 * NC, 0:NI] = jnp.where(odd, before[:NC], 0.0)
    forward[2 * NC : 3 * NC, 2 * NI :] = jnp.where(odd, 0.0, -after[NC:])
    forward[3 * NC :, 0:NI] = jnp.where(odd, before[NC:], 0.0) - first0[:NC]
    forward[3 * NC :, NI : 2 * NI] = last0[:NC]
    backward[...] = jnp.zeros_like(backward)
    backward[0:NC, :] = forward[0:NC, :]
    backward[NC : 2 * NC, NI : 2 * NI] = -first1[NC:]
    backward[NC : 2 * NC, 2 * NI :] = last1[NC:] - after[:NC]
    backward[2 * NC : 3 * NC, 0:NI] = jnp.where(odd, 0.0, before[:NC])
    backward[2 * NC : 3 * NC, 2 * NI :] = jnp.where(odd, -after[NC:], 0.0)
    backward[3 * NC :, 0:NI] = jnp.where(odd, 0.0, before[NC:] - first0[:NC])
    backward[3 * NC :, NI : 2 * NI] = last0[:NC]

    keep_split(forward_parts, forward[...])
    keep_split(backward_parts, backward[...])
    keep_split(coarse_parts, coarse[...])

    def coarse_solve(at):
        all_but_one(gathered, at, wide_recv.at[at]).wait()
        assembled = []
        for j in range(n // 2):
            low = jnp.where(lane < 64, gathered[at, 2 * j], gathered[at, (2 * j + 2) % n])
            high = jnp.where(lane >= 32, gathered[at, 2 * j + 1], gathered[at, (2 * j - 1) % n])
            assembled.append(low + high)
        return split_dot(jnp.concatenate(assembled, axis=1), coarse_parts, 1)

    def jumps(fields, across):
        first, second = fields
        left = jnp.where(odd, across, 0.0) - first[:, :NI]
        right = second[:, unknowns - NI :] - jnp.where(odd, 0.0, across)
        return jnp.concatenate([left, first[:, unknowns - NI :] - second[:, :NI], right], axis=1)

    per_piece = unknowns // n
    width = sub_count * per_piece

    def piece_part(fields, which, p):
        block = p * per_piece // LANES
        inside = p * per_piece % LANES
        part = jnp.zeros((8, LANES), jnp.float32)
        for k in range(sub_count):
            target = which * width + k * per_piece
            rolled = pltpu.roll(
                fields[k][:, block * LANES : (block + 1) * LANES], (target - inside) % LANES, 1
            )
            part = jnp.where((lane >= target) & (lane < target + per_piece), rolled, part)
        return part

    solved = coarse_solve(0)
    met.wait_recv()
    vector0 = jumps(local, edge[0]) + split_dot(solved, forward_parts, 0)

    def start_image(vector, at):
        gathered[at, me] = placed(split_dot(vector, backward_parts, 1))
        broadcast(gathered, at, at)
        slot = 2 * at - 1
        edge_out[slot] = jnp.where(odd, vector[:, 2 * NI :], vector[:, :NI])
        copy = remote(edge_out.at[slot], edge.at[slot], edge_send.at[slot], edge_recv.at[slot], outward)
        copy.start()
        edges.append(copy)
        left, middle, right = vector[:, :NI], vector[:, NI : 2 * NI], vector[:, 2 * NI :]
        near = rr.at[jnp.where(odd, 0, 1)]
        facing = nn(jnp.where(odd, -left, -middle), near[:NI, :]) + nn(
            jnp.where(odd, middle, right), near[unknowns - NI :, :]
        )
        return copy, facing_edge(facing[:, :NI], facing[:, unknowns - NI :], slot + 1), facing

    def whole(vector, copy, at):
        copy.wait_recv()
        other = edge[2 * at - 1]
        return jnp.concatenate(
            [
                vector[:, :NI] + jnp.where(odd, 0.0, other),
                vector[:, NI : 2 * NI],
                vector[:, 2 * NI :] + jnp.where(odd, other, 0.0),
            ],
            axis=1,
        )

    def end_image(full, met, facing, at):
        left, middle, right = full[:, :NI], full[:, NI : 2 * NI], full[:, 2 * NI :]
        far = rr.at[jnp.where(odd, 1, 0)]
        outer_field = nn(jnp.where(odd, -middle, -left), far[:NI, :]) + nn(
            jnp.where(odd, right, middle), far[unknowns - NI :, :]
        )
        inside = [jnp.where(odd, facing, outer_field), jnp.where(odd, outer_field, facing)]
        met.wait_recv()
        known = jumps(inside, edge[2 * at])
        values = coarse_solve(at)
        return inside, values, known + split_dot(values, forward_parts, 0)

    def counted(vector):
        return jnp.concatenate([jnp.where(odd, 0.0, vector[:, :NI]), vector[:, NI:]], axis=1)

    def with_corners(inside, values):
        return [
            inside[k] + nn(values, corner[:, k * unknowns : (k + 1) * unknowns]) for k in range(sub_count)
        ]

    def column(values):
        return jnp.sum(values, axis=1, keepdims=True)

    sent0, met0, facing0 = start_image(vector0, 1)
    first_fields = with_corners(local, solved)
    for k in range(sub_count):
        green[k] = first_fields[k]
    for p in range(n):
        pieces[p] = piece_part(first_fields, 0, p)
    full0 = whole(vector0, sent0, 1)
    inside0, values0, vector1 = end_image(full0, met0, facing0, 1)

    sent1, met1, facing1 = start_image(vector1, 2)
    norm_row = jnp.where(lane == sublane, column(full0 * counted(vector0)), 0.0) + jnp.where(
        lane == sublane + 8, column(full0 * counted(vector1)), 0.0
    )
    norms[0, me] = jnp.sum(norm_row, axis=0, keepdims=True)
    broadcast(norms, 0, 3)
    fields0 = with_corners(inside0, values0)
    for p in range(n):
        pieces[p] = pieces[p] + piece_part(fields0, 1, p)
    load_basis.wait()
    keep_split(basis_parts, basis[...])
    full1 = whole(vector1, sent1, 2)
    inside1, values1, vector2 = end_image(full1, met1, facing1, 2)
    fields1 = with_corners(inside1, values1)

    all_but_one(norms, 0, wide_recv.at[3]).wait()
    totals = jnp.broadcast_to(jnp.sum(norms[0], axis=0), (8, LANES))
    norm0 = column(jnp.where(lane == sublane, totals, 0.0))
    curve0 = column(jnp.where(lane == sublane + 8, totals, 0.0))
    alpha0 = norm0 / curve0
    residual = full0 - alpha0 * full1
    residual_part = counted(vector0 - alpha0 * vector1)
    residual_image = counted(vector1 - alpha0 * vector2)
    extra = (
        jnp.where(lane == 3 * width, column(residual * residual_part), 0.0)
        + jnp.where(lane == 3 * width + 1, column(residual * residual_image), 0.0)
        + jnp.where(lane == 3 * width + 2, column(residual * counted(vector1)), 0.0)
    )
    for p in range(n):
        pieces[p] = pieces[p] + piece_part(fields1, 2, p) + extra
    for t in range(n):
        outgoing[t] = pieces[inverse[t]]

    def send_piece(rank):
        remote(outgoing.at[rank], incoming.at[0, me], wide_send.at[4], wide_recv.at[4], rank).start()

    others(send_piece)
    incoming[0, me] = outgoing[me]
    all_but_one(incoming, 0, wide_recv.at[4]).wait()

    sums = jnp.sum(incoming[0], axis=0)
    norm1 = column(jnp.where(lane == 3 * width, sums, 0.0))
    curve_rr = column(jnp.where(lane == 3 * width + 1, sums, 0.0))
    curve_rp = column(jnp.where(lane == 3 * width + 2, sums, 0.0))
    beta = norm1 / norm0
    curve1 = curve_rr + 2.0 * beta * curve_rp + beta * beta * curve0
    alpha1 = norm1 / curve1
    scale0 = alpha0 + alpha1 * (1.0 + beta)
    scale1 = -alpha1 * alpha0

    factor = jnp.where(lane < width, 1.0, jnp.where(lane < 2 * width, -scale0, -scale1))
    factor = jnp.where(lane < 3 * width, factor, 0.0)
    per_tile = LANES // width
    snapshot_tiles = []
    for j in range(n // per_tile):
        tile = jnp.zeros((8, LANES), jnp.float32)
        for i in range(per_tile):
            scaled = incoming[0, j * per_tile + i] * factor
            total = scaled
            for which in (1, 2):
                total = total + pltpu.roll(scaled, LANES - which * width, 1)
            if i:
                total = pltpu.roll(total, i * width, 1)
            tile = jnp.where((lane >= i * width) & (lane < (i + 1) * width), total, tile)
        snapshot_tiles.append(tile)
    snapshots = jnp.concatenate(snapshot_tiles, axis=1)
    proj_parts[seat] = split_dot(snapshots, basis_parts, 0)
    for i in range(1, inner):
        rank = plane * inner + lax.rem(seat + i, inner)
        remote(proj_parts.at[seat], proj_parts.at[seat], wide_send.at[5], wide_recv.at[5], rank).start()

    for k in range(sub_count):
        carried = green[k] - scale0 * fields0[k] - scale1 * fields1[k]
        now, vel, acc = disp_now[:, k, :], vel_now[:, k, :], acc_now[:, k, :]
        accel_new = (
            (carried - now) / (newmark_beta * time_step * time_step)
            - vel / (newmark_beta * time_step)
            - (0.5 / newmark_beta - 1.0) * acc
        )
        disp_out[:, k, :] = carried
        vel_out[:, k, :] = vel + time_step * ((1.0 - newmark_gamma) * acc + newmark_gamma * accel_new)

    pltpu.make_async_copy(
        proj_parts.at[pl.ds(0, inner - 1)], proj_parts.at[pl.ds(0, inner - 1)], wide_recv.at[5]
    ).wait()
    proj_sums[plane] = jnp.sum(proj_parts[...], axis=0)
    for i in range(1, outer):
        rank = lax.rem(plane + i, outer) * inner + seat
        remote(proj_sums.at[plane], proj_sums.at[plane], wide_send.at[7], wide_recv.at[7], rank).start()
    pltpu.make_async_copy(
        proj_sums.at[pl.ds(0, outer - 1)], proj_sums.at[pl.ds(0, outer - 1)], wide_recv.at[7]
    ).wait()
    projection = jnp.sum(proj_sums[...], axis=0)
    proj_out[...] = projection
    remainder = snapshots - split_dot(projection, basis_parts, 1)
    gram_row = jnp.zeros((8, LANES), jnp.float32)
    for shift in range(5):
        product = remainder * pltpu.roll(remainder, shift, 0)
        other = lax.rem(sublane + 8 - shift, 8)
        here = (lane == 8 * sublane + other) | ((lane == 8 * other + sublane) & (shift < 4))
        gram_row = jnp.where(here, column(product), gram_row)
    gram_parts[0, me] = jnp.sum(gram_row, axis=0, keepdims=True)
    broadcast(gram_parts, 0, 6)
    all_but_one(gram_parts, 0, wide_recv.at[6]).wait()
    gram_row = jnp.broadcast_to(jnp.sum(gram_parts[0], axis=0), (8, LANES))
    work = gram_row
    for i in range(1, 8):
        work = jnp.where(sublane == i, pltpu.roll(gram_row, LANES - 8 * i, 1), work)
    for j in range(8):
        inverse_root = lax.rsqrt(work[j : j + 1, j : j + 1])
        pivot = work[j : j + 1, :] * inverse_root
        below = work[:, j : j + 1] * inverse_root
        pivot_rows = remainder[j : j + 1, :] * inverse_root
        work = jnp.where(sublane == j, pivot, jnp.where(sublane > j, work - below * pivot, work))
        row_at = lax.broadcasted_iota(jnp.int32, remainder.shape, 0)
        remainder = jnp.where(
            row_at == j, pivot_rows, jnp.where(row_at > j, remainder - below * pivot_rows, remainder)
        )
    scale_rows = math.sqrt(snapshots.shape[1] * n)
    r_out[...] = jnp.where(lane >= sublane, work, 0.0)[:, :8] * (1.0 / scale_rows)
    cols_out[...] = remainder * scale_rows

    for copy in halos + edges:
        copy.wait_send()
    for at in range(3):
        all_but_one(gathered, at, wide_send.at[at]).wait()
    all_but_one(norms, 0, wide_send.at[3]).wait()
    all_but_one(incoming, 0, wide_send.at[4]).wait()
    pltpu.make_async_copy(
        proj_parts.at[pl.ds(0, inner - 1)], proj_parts.at[pl.ds(0, inner - 1)], wide_send.at[5]
    ).wait()
    pltpu.make_async_copy(
        proj_sums.at[pl.ds(0, outer - 1)], proj_sums.at[pl.ds(0, outer - 1)], wide_send.at[7]
    ).wait()
    all_but_one(gram_parts, 0, wide_send.at[6]).wait()


def solution(mesh):
    groups = mesh.shape["grp"]
    n = mesh.shape["sub"] * groups
    inner = math.gcd(n, 8)

    def shards(
        rr_inverse,
        corner_modes,
        coarse_inverse,
        inertia,
        disp_now,
        vel_now,
        acc_now,
        load_next,
        basis_rows,
        piece_owner,
    ):
        case_count, sub_count, unknowns = disp_now.shape
        rank = basis_rows.shape[1]
        local_rows = basis_rows.shape[0]
        width = (sub_count + 2) * NC
        f32 = jnp.float32
        vmem = pl.BlockSpec(memory_space=pltpu.VMEM)
        anywhere = pl.BlockSpec(memory_space=pl.ANY)
        results = (
            jax.ShapeDtypeStruct(disp_now.shape, f32),
            jax.ShapeDtypeStruct(disp_now.shape, f32),
            jax.ShapeDtypeStruct((case_count, rank), f32),
            jax.ShapeDtypeStruct((case_count, case_count), f32),
            jax.ShapeDtypeStruct((case_count, local_rows), f32),
        )
        computed = pl.pallas_call(
            functools.partial(kernel, n, groups, inner),
            out_shape=results,
            in_specs=[anywhere] * 10,
            out_specs=(vmem,) * 5,
            scratch_shapes=[
                pltpu.SMEM(piece_owner.shape, jnp.int32),
                pltpu.SMEM(piece_owner.shape, jnp.int32),
                pltpu.VMEM(inertia.shape, f32),
                pltpu.VMEM(disp_now.shape, f32),
                pltpu.VMEM(vel_now.shape, f32),
                pltpu.VMEM(acc_now.shape, f32),
                pltpu.VMEM(load_next.shape, f32),
                pltpu.VMEM((3, width, coarse_inverse.shape[1]), jnp.bfloat16),
                pltpu.VMEM((3, width, (sub_count + 1) * NI), jnp.bfloat16),
                pltpu.VMEM((3, width, (sub_count + 1) * NI), jnp.bfloat16),
                pltpu.VMEM((3,) + basis_rows.shape, jnp.bfloat16),
                pltpu.VMEM(rr_inverse.shape, f32),
                pltpu.VMEM(corner_modes.shape, f32),
                pltpu.VMEM((width, coarse_inverse.shape[1]), f32),
                pltpu.VMEM(basis_rows.shape, f32),
                pltpu.VMEM((2 * NC, NI), f32),
                pltpu.VMEM((2 * NC, NI), f32),
                pltpu.VMEM((width, sub_count * unknowns), f32),
                pltpu.VMEM((width, (sub_count + 1) * NI), f32),
                pltpu.VMEM((width, (sub_count + 1) * NI), f32),
                pltpu.VMEM((3, n, case_count, width), f32),
                pltpu.VMEM((5, case_count, NI), f32),
                pltpu.VMEM((5, case_count, NI), f32),
                pltpu.VMEM((1, n, 1, LANES), f32),
                pltpu.VMEM((n, case_count, LANES), f32),
                pltpu.VMEM((n, case_count, LANES), f32),
                pltpu.VMEM((1, n, case_count, LANES), f32),
                pltpu.VMEM((inner, case_count, rank), f32),
                pltpu.VMEM((n // inner, case_count, rank), f32),
                pltpu.VMEM((1, n, 1, LANES), f32),
                pltpu.VMEM((sub_count, case_count, unknowns), f32),
                pltpu.SemaphoreType.DMA((10,)),
                pltpu.SemaphoreType.DMA((4,)),
                pltpu.SemaphoreType.DMA((4,)),
                pltpu.SemaphoreType.DMA((8,)),
                pltpu.SemaphoreType.DMA((8,)),
                pltpu.SemaphoreType.DMA((5,)),
                pltpu.SemaphoreType.DMA((5,)),
            ],
            compiler_params=pltpu.CompilerParams(collective_id=0, has_side_effects=True),
        )(
            piece_owner,
            rr_inverse,
            corner_modes,
            coarse_inverse,
            basis_rows,
            inertia,
            disp_now,
            vel_now,
            acc_now,
            load_next,
        )
        disp, vel, proj, r_factor, columns = pl.pallas_call(
            hand_over, out_shape=results, in_specs=[vmem] * 5, out_specs=(vmem,) * 5
        )(*computed)
        return disp, vel, proj.T, r_factor, columns

    return jax.shard_map(
        shards,
        mesh=mesh,
        in_specs=(
            P(("sub", "grp"), None, None),
            P(("sub", "grp"), None, None),
            P(("sub", "grp"), None),
            P(("sub", "grp"), None),
            P(None, ("sub", "grp"), None),
            P(None, ("sub", "grp"), None),
            P(None, ("sub", "grp"), None),
            P(None, ("sub", "grp"), None),
            P(("sub", "grp"), None),
            P(),
        ),
        out_specs=(
            P(None, ("sub", "grp"), None),
            P(None, ("sub", "grp"), None),
            P(),
            P(),
            P(None, ("sub", "grp")),
        ),
        check_vma=False,
    )
```

```python
import functools
import math

import jax
import jax.numpy as jnp
from jax import lax
from jax.experimental import pallas as pl
from jax.experimental.pallas import tpu as pltpu
from jax.sharding import PartitionSpec as P

NC = 32
NI = 128
LANES = 128

time_step = 0.5
newmark_beta = 0.25
newmark_gamma = 0.5

MESH = pl.DeviceIdType.MESH


def nn(a, b):
    return lax.dot_general(
        a, b, (((1,), (0,)), ((), ())), precision=lax.Precision.HIGHEST, preferred_element_type=jnp.float32
    )


def nt(a, b):
    return lax.dot_general(
        a, b, (((1,), (1,)), ((), ())), precision=lax.Precision.HIGHEST, preferred_element_type=jnp.float32
    )


def split(x):
    first = x.astype(jnp.bfloat16)
    return first, (x - first.astype(jnp.float32)).astype(jnp.bfloat16)


def keep_split(parts, matrix, at=0):
    for which, part in enumerate(split(matrix)):
        parts[which, at : at + matrix.shape[0]] = part


def split_dot(x, parts, contracted):
    first, second = split(x)
    rows = x.shape[0]

    def product(a, b):
        return lax.dot_general(a, b, (((1,), (contracted,)), ((), ())), preferred_element_type=jnp.float32)

    large = product(jnp.concatenate([first, second], axis=0), parts[0])
    return large[:rows] + (large[rows:] + product(first, parts[1]))


def hand_over(*refs):
    half = len(refs) // 2
    for source, target in zip(refs[:half], refs[half:]):
        target[...] = source[...]


def kernel(
    n,
    groups,
    inner,
    owner_hbm,
    rr_hbm,
    modes_hbm,
    coarse_hbm,
    basis_hbm,
    inertia_hbm,
    disp_hbm,
    vel_hbm,
    acc_hbm,
    load_hbm,
    disp_out,
    vel_out,
    proj_out,
    r_out,
    cols_out,
    owner,
    inverse,
    inertia,
    disp_now,
    vel_now,
    acc_now,
    load_next,
    coarse_parts,
    early_parts,
    step_parts,
    known_parts,
    backward_parts,
    corner_parts,
    basis_parts,
    rr,
    modes,
    coarse,
    basis,
    modes_next,
    modes_prev,
    corner,
    forward,
    backward,
    inward,
    outgo,
    gathered,
    edge,
    edge_out,
    norms,
    pieces,
    outgoing,
    incoming,
    proj_parts,
    proj_sums,
    gram_parts,
    green,
    local_sem,
    const_send,
    const_recv,
    wide_send,
    wide_recv,
    edge_send,
    edge_recv,
):
    sub_count, unknowns = rr.shape[0], rr.shape[1]
    rows = sub_count * NC
    me = lax.axis_index("sub") * groups + lax.axis_index("grp")
    following = lax.rem(me + 1, n)
    earlier = lax.rem(me + n - 1, n)
    odd = lax.rem(me, 2) == 1
    partner = jnp.where(odd, earlier, following)
    outward = jnp.where(odd, following, earlier)

    def device(rank):
        return (rank // groups, lax.rem(rank, groups))

    plane, outer = me // inner, n // inner
    seat = lax.rem(me, inner)
    seats = [lax.rem(2 * inner - 1 - seat + i, inner) for i in range(inner)]
    mirrored = 2 * plane > outer - 1
    depth = jnp.where(mirrored, outer - 1 - plane, plane)
    lead = outer - 1 - 2 * depth

    def others(body):
        def step(i, carry):
            beyond = i - lead
            turn = jnp.where(lax.rem(beyond, 2) == 0, 2 * depth - beyond // 2, beyond // 2)
            at = jnp.where(i < lead, outer - 1 - i, turn)
            at = jnp.where(mirrored, outer - 1 - at, at)
            for there in seats:
                body(at * inner + there)
            return carry

        lax.fori_loop(0, outer - 1, step, 0)
        for i in range(1, inner):
            body(plane * inner + lax.rem(seat + i, inner))

    def remote(src, dst, send, recv, rank):
        return pltpu.make_async_remote_copy(
            src_ref=src, dst_ref=dst, send_sem=send, recv_sem=recv, device_id=device(rank), device_id_type=MESH
        )

    barrier = pltpu.get_barrier_semaphore()
    others(lambda rank: pl.semaphore_signal(barrier, inc=1, device_id=device(rank), device_id_type=MESH))

    load_rr = pltpu.make_async_copy(rr_hbm, rr, local_sem.at[0])
    load_modes = pltpu.make_async_copy(modes_hbm, modes, local_sem.at[1])
    load_coarse = pltpu.make_async_copy(coarse_hbm, coarse.at[pl.ds(0, rows)], local_sem.at[2])
    load_basis = pltpu.make_async_copy(basis_hbm, basis, local_sem.at[3])
    fields_in = [
        pltpu.make_async_copy(source, target, local_sem.at[4 + at])
        for at, (source, target) in enumerate(
            (
                (inertia_hbm, inertia),
                (disp_hbm, disp_now),
                (vel_hbm, vel_now),
                (acc_hbm, acc_now),
                (load_hbm, load_next),
            )
        )
    ]
    load_owner = pltpu.make_async_copy(owner_hbm, owner, local_sem.at[9])
    load_modes.start()
    for copy in fields_in:
        copy.start()
    load_owner.start()
    load_coarse.start()
    load_rr.start()
    load_basis.start()

    lane = lax.broadcasted_iota(jnp.int32, (8, LANES), 1)
    sublane = lax.broadcasted_iota(jnp.int32, (8, LANES), 0)

    def right_side(k):
        return load_next[:, k, :] + inertia[k : k + 1, :] * (
            disp_now[:, k, :]
            + time_step * vel_now[:, k, :]
            + (0.5 - newmark_beta) * time_step * time_step * acc_now[:, k, :]
        )

    for copy in fields_in:
        copy.wait()
    sides = [right_side(k) for k in range(sub_count)]

    corner[...] = jnp.zeros_like(corner)
    load_modes.wait()
    corner[0:NC, 0:unknowns] = modes[0, NC:, :]
    corner[0:NC, unknowns:] = modes[1, :NC, :]
    corner[NC : 2 * NC, unknowns:] = modes[1, NC:, :]
    corner[3 * NC :, 0:unknowns] = modes[0, :NC, :]

    def placed(tile):
        return jnp.where(odd, pltpu.roll(tile, 64, 1), tile)

    def broadcast(buffer, at, sem):
        def send(rank):
            remote(buffer.at[at, me], buffer.at[at, me], wide_send.at[sem], wide_recv.at[sem], rank).start()

        others(send)

    def all_but_one(buffer, at, sem):
        return pltpu.make_async_copy(buffer.at[at, pl.ds(0, n - 1)], buffer.at[at, pl.ds(0, n - 1)], sem)

    gathered[0, me] = placed(nt(jnp.concatenate(sides, axis=1), corner[...]))

    pl.semaphore_wait(barrier, n - 1)
    next_modes = [
        remote(modes.at[k, :, pl.ds(start, NI)], modes_next.at[at], const_send.at[at], const_recv.at[at], earlier)
        for at, (k, start) in enumerate(((0, 0), (0, unknowns - NI), (1, 0)))
    ]
    halos = next_modes + [
        remote(modes.at[1, :, pl.ds(unknowns - NI, NI)], modes_prev, const_send.at[3], const_recv.at[3], following)
    ]
    broadcast(gathered, 0, 0)
    for copy in halos:
        copy.start()
    load_coarse.wait()
    coarse_near = [
        remote(
            coarse.at[pl.ds(k * NC, NC)], coarse.at[pl.ds(slot * NC, NC)], const_send.at[4 + k], const_recv.at[4 + k], partner
        )
        for k, slot in ((0, 2), (1, 4))
    ]
    coarse_far = remote(
        coarse.at[pl.ds(NC, NC)], coarse.at[pl.ds(3 * NC, NC)], const_send.at[6], const_recv.at[6], following
    )
    for copy in coarse_near + [coarse_far]:
        copy.start()

    load_rr.wait()
    local = [nn(sides[k], rr[k]) for k in range(sub_count)]
    def facing_edge(first, last, at):
        edge_out[at] = jnp.where(odd, first, last)
        copy = remote(edge_out.at[at], edge.at[at], edge_send.at[at], edge_recv.at[at], partner)
        copy.start()
        edges.append(copy)
        return copy

    edges = []
    met = facing_edge(local[0][:, :NI], local[1][:, unknowns - NI :], 0)
    middle_known = local[0][:, unknowns - NI :] - local[1][:, :NI]
    met_middle = facing_edge(middle_known, middle_known, 5)

    load_owner.wait()

    def find(t, carry):
        at = jnp.int32(0)
        for p in range(n):
            at = jnp.where(owner[p] == t, p, at)
        inverse[t] = at
        return carry

    lax.fori_loop(0, n, find, 0)
    keep_split(corner_parts, corner[...])
    keep_split(coarse_parts, coarse[0:rows])
    for copy in coarse_near:
        copy.wait_recv()
    keep_split(coarse_parts, coarse[2 * NC : 3 * NC], 2 * NC)
    keep_split(coarse_parts, coarse[4 * NC :], 3 * NC)
    for copy in halos:
        copy.wait_recv()
    first0, last0 = modes[0, :, :NI], modes[0, :, unknowns - NI :]
    first1, last1 = modes[1, :, :NI], modes[1, :, unknowns - NI :]
    before, after, after_last, after_first1 = modes_prev[...], modes_next[0], modes_next[1], modes_next[2]
    jump = {
        (-1, -2): before[:NC],
        (-1, -1): before[NC:] - first0[:NC],
        (-1, 0): -first0[NC:],
        (0, -1): last0[:NC],
        (0, 0): last0[NC:] - first1[:NC],
        (0, 1): -first1[NC:],
        (1, 0): last1[:NC],
        (1, 1): last1[NC:] - after[:NC],
        (1, 2): -after[NC:],
        (2, 1): after_last[:NC],
        (2, 2): after_last[NC:] - after_first1[:NC],
        (2, 3): -after_first1[NC:],
    }
    for row, at_even, at_odd in ((0, 0, 0), (1, 1, 1), (2, 2, -2), (3, 3, -1)):
        for i in range(-1, 3):
            for target, (one, two) in ((inward, (at_even, at_odd)), (outgo, (at_odd, at_even))):
                even_block, odd_block = jump.get((i, one), 0.0), jump.get((i, two), 0.0)
                target[row * NC : (row + 1) * NC, (i + 1) * NI : (i + 2) * NI] = jnp.broadcast_to(
                    even_block if one == two else jnp.where(odd, odd_block, even_block), (NC, NI)
                )
    nothing = jnp.zeros((2 * NC, NI), jnp.float32)
    leaving = jnp.where(odd, last1, jnp.concatenate([-first0[NC:], nothing[:NC]], axis=0))
    added = jnp.where(odd, jnp.concatenate([nothing[:NC], -after[:NC]], axis=0), 0.0)
    keep_split(
        early_parts,
        jnp.concatenate(
            [
                nt(inward[...], outgo[...]),
                jnp.concatenate([leaving, nothing], axis=0),
                jnp.concatenate([added, nothing], axis=0),
            ],
            axis=1,
        ),
    )
    keep_split(known_parts, outgo[...])
    forward[...] = jnp.zeros_like(forward)
    forward[0:NC, 0:NI] = -first0[NC:]
    forward[0:NC, NI : 2 * NI] = last0[NC:] - first1[:NC]
    forward[0:NC, 2 * NI :] = last1[:NC]
    forward[NC : 2 * NC, NI : 2 * NI] = -first1[NC:]
    forward[NC : 2 * NC, 2 * NI :] = last1[NC:] - jnp.where(odd, 0.0, after[:NC])
    forward[2 * NC : 3 * NC, 0:NI] = jnp.where(odd, before[:NC], 0.0)
    forward[2 * NC : 3 * NC, 2 * NI :] = jnp.where(odd, 0.0, -after[NC:])
    forward[3 * NC :, 0:NI] = jnp.where(odd, before[NC:], 0.0) - first0[:NC]
    forward[3 * NC :, NI : 2 * NI] = last0[:NC]
    backward[...] = jnp.zeros_like(backward)
    backward[0:NC, :] = forward[0:NC, :]
    backward[NC : 2 * NC, NI : 2 * NI] = -first1[NC:]
    backward[NC : 2 * NC, 2 * NI :] = last1[NC:] - after[:NC]
    backward[2 * NC : 3 * NC, 0:NI] = jnp.where(odd, 0.0, before[:NC])
    backward[2 * NC : 3 * NC, 2 * NI :] = jnp.where(odd, -after[NC:], 0.0)
    backward[3 * NC :, 0:NI] = jnp.where(odd, 0.0, before[NC:] - first0[:NC])
    backward[3 * NC :, NI : 2 * NI] = last0[:NC]

    keep_split(step_parts, jnp.concatenate([forward[...], nt(forward[...], backward[...])], axis=1))
    keep_split(backward_parts, backward[...])

    def assemble(at):
        all_but_one(gathered, at, wide_recv.at[at]).wait()
        assembled = []
        for j in range(n // 2):
            low = jnp.where(lane < 64, gathered[at, 2 * j], gathered[at, (2 * j + 2) % n])
            high = jnp.where(lane >= (64 if at == 1 else 32), gathered[at, 2 * j + 1], gathered[at, (2 * j - 1) % n])
            assembled.append(low + high)
        return jnp.concatenate(assembled, axis=1)

    def coarse_solve(at):
        return split_dot(assemble(at), coarse_parts, 1)

    def jumps(fields, across):
        first, second = fields
        left = jnp.where(odd, across, 0.0) - first[:, :NI]
        right = second[:, unknowns - NI :] - jnp.where(odd, 0.0, across)
        return jnp.concatenate([left, first[:, unknowns - NI :] - second[:, :NI], right], axis=1)

    per_piece = unknowns // n
    width = sub_count * per_piece
    per_tile = LANES // width
    spot = lax.rem(me, per_tile)

    def piece_part(fields, which, p):
        block = p * per_piece // LANES
        inside = p * per_piece % LANES
        start = lax.rem(spot + which, per_tile) * width
        part = jnp.zeros((8, LANES), jnp.float32)
        for k in range(sub_count):
            target = start + k * per_piece
            rolled = pltpu.roll(
                fields[k][:, block * LANES : (block + 1) * LANES], lax.rem(target + LANES - inside, LANES), 1
            )
            part = jnp.where((lane >= target) & (lane < target + per_piece), rolled, part)
        return part

    def outer_half(vector, at):
        slot = 2 * at - 1
        edge_out[slot] = vector
        copy = remote(edge_out.at[slot], edge.at[slot], edge_send.at[slot], edge_recv.at[slot], outward)
        copy.start()
        edges.append(copy)
        return copy

    def send_terms(terms, at):
        gathered[at, me] = placed(terms)
        broadcast(gathered, at, at)

    def outermost(vector):
        return jnp.where(odd, vector[:, 2 * NI : 3 * NI], vector[:, :NI])

    def facing_field(vector, at):
        left, middle, right = vector[:, :NI], vector[:, NI : 2 * NI], vector[:, 2 * NI :]
        near = rr.at[jnp.where(odd, 0, 1)]
        facing = nn(jnp.where(odd, -left, -middle), near[:NI, :]) + nn(
            jnp.where(odd, middle, right), near[unknowns - NI :, :]
        )
        return facing_edge(facing[:, :NI], facing[:, unknowns - NI :], 2 * at), facing

    met.wait_recv()
    known = jumps(local, edge[0])
    met_middle.wait_recv()
    carried = split_dot(jnp.concatenate([known, jnp.where(odd, 0.0, edge[5])], axis=1), known_parts, 1)
    assembled = assemble(0)
    solved = split_dot(assembled, coarse_parts, 1)
    early = split_dot(solved, early_parts, 0)
    sent0 = outer_half(outermost(known) + early[:, LANES : LANES + NI], 1)
    send_terms(carried + early[:, :LANES], 1)
    extra = early[:, LANES + NI :]
    coarse_far.wait_recv()
    keep_split(coarse_parts, coarse[3 * NC : 4 * NC], 3 * NC)
    solved = jnp.concatenate([solved[:, : 3 * NC], split_dot(assembled, coarse_parts.at[:, pl.ds(3 * NC, NC)], 1)], axis=1)
    vector0 = known + split_dot(solved, step_parts, 0)[:, : 3 * NI]
    met0, facing0 = facing_field(vector0, 1)

    def whole(vector, copy, at, extra=0.0):
        copy.wait_recv()
        other = edge[2 * at - 1] + extra
        return jnp.concatenate(
            [
                vector[:, :NI] + jnp.where(odd, 0.0, other),
                vector[:, NI : 2 * NI],
                vector[:, 2 * NI :] + jnp.where(odd, other, 0.0),
            ],
            axis=1,
        )

    def end_image(full, met, facing, at):
        left, middle, right = full[:, :NI], full[:, NI : 2 * NI], full[:, 2 * NI :]
        far = rr.at[jnp.where(odd, 1, 0)]
        outer_field = nn(jnp.where(odd, -middle, -left), far[:NI, :]) + nn(
            jnp.where(odd, right, middle), far[unknowns - NI :, :]
        )
        inside = [jnp.where(odd, facing, outer_field), jnp.where(odd, outer_field, facing)]
        met.wait_recv()
        known = jumps(inside, edge[2 * at])
        carried = split_dot(known, backward_parts, 1)
        return inside, known, carried, coarse_solve(at)

    def counted(vector):
        return jnp.concatenate([jnp.where(odd, 0.0, vector[:, :NI]), vector[:, NI:]], axis=1)

    def with_corners(inside, values):
        added = split_dot(values, corner_parts, 0)
        return [inside[k] + added[:, k * unknowns : (k + 1) * unknowns] for k in range(sub_count)]

    def column(values):
        return jnp.sum(values, axis=1, keepdims=True)

    first_fields = with_corners(local, solved)
    for k in range(sub_count):
        green[k] = first_fields[k]
    for p in range(n):
        pieces[p] = piece_part(first_fields, 0, p)
    full0 = whole(vector0, sent0, 1, extra)
    inside0, known, carried, values0 = end_image(full0, met0, facing0, 1)

    step = split_dot(values0, step_parts, 0)
    vector1 = known + step[:, : 3 * NI]
    sent1 = outer_half(outermost(vector1), 2)
    send_terms(carried + step[:, 3 * NI :], 2)
    norm_row = jnp.where(lane == sublane, column(full0 * counted(vector0)), 0.0) + jnp.where(
        lane == sublane + 8, column(full0 * counted(vector1)), 0.0
    )
    norms[0, me] = jnp.sum(norm_row, axis=0, keepdims=True)
    broadcast(norms, 0, 3)
    met1, facing1 = facing_field(vector1, 2)
    fields0 = with_corners(inside0, values0)
    for p in range(n):
        pieces[p] = pieces[p] + piece_part(fields0, 1, p)
    load_basis.wait()
    keep_split(basis_parts, basis[...])
    full1 = whole(vector1, sent1, 2)
    weighed0, weighed1 = [
        split_dot(counted(full), step_parts.at[:, :, pl.ds(0, 3 * NI)], 1) for full in (full0, full1)
    ]
    inside1, known, carried, values1 = end_image(full1, met1, facing1, 2)
    fields1 = with_corners(inside1, values1)

    all_but_one(norms, 0, wide_recv.at[3]).wait()
    totals = jnp.broadcast_to(jnp.sum(norms[0], axis=0), (8, LANES))
    norm0, curve0 = [column(jnp.where(lane == sublane + 8 * which, totals, 0.0)) for which in range(2)]
    alpha0 = norm0 / curve0
    residual = counted(full0 - alpha0 * full1)
    free = lax.rem(spot + 3, per_tile) * width + per_piece
    extra = (
        jnp.where(lane == free, column(residual * (vector0 - alpha0 * vector1)), 0.0)
        + jnp.where(
            lane == free + 1,
            column(residual * (vector1 - alpha0 * known))
            - alpha0 * column((weighed0 - alpha0 * weighed1) * values1),
            0.0,
        )
        + jnp.where(lane == free + 2, column(residual * vector1), 0.0)
    )
    for p in range(n):
        pieces[p] = pieces[p] + piece_part(fields1, 2, p) + extra
    for t in range(n):
        outgoing[t] = pieces[inverse[t]]

    def send_piece(rank):
        remote(outgoing.at[rank], incoming.at[0, me], wide_send.at[4], wide_recv.at[4], rank).start()

    others(send_piece)
    incoming[0, me] = outgoing[me]
    all_but_one(incoming, 0, wide_recv.at[4]).wait()
    gathered_sums = jnp.zeros((8, LANES), jnp.float32)
    for i in range(per_tile):
        total = incoming[0, i]
        for j in range(1, n // per_tile):
            total = total + incoming[0, j * per_tile + i]
        at = (i + 3) % per_tile * width + per_piece
        gathered_sums = jnp.where((lane >= at) & (lane < at + 3), total, gathered_sums)
    norm1, curve_rr, curve_rp = [
        column(jnp.where(lax.rem(lane, width) == per_piece + which, gathered_sums, 0.0)) for which in range(3)
    ]
    beta = norm1 / norm0
    curve1 = curve_rr + 2.0 * beta * curve_rp + beta * beta * curve0
    alpha1 = norm1 / curve1
    scale0 = alpha0 + alpha1 * (1.0 + beta)
    scale1 = -alpha1 * alpha0

    snapshot_tiles = []
    for j in range(n // per_tile):
        total = jnp.zeros((8, LANES), jnp.float32)
        for which, factor in enumerate((1.0, -scale0, -scale1)):
            tile = incoming[0, j * per_tile]
            for i in range(1, per_tile):
                block = (i + which) % per_tile
                inside = (lane >= block * width) & (lane < (block + 1) * width)
                tile = jnp.where(inside, incoming[0, j * per_tile + i], tile)
            if which:
                tile = pltpu.roll(tile, LANES - which * width, 1)
            total = total + factor * tile
        snapshot_tiles.append(total)
    snapshots = jnp.concatenate(snapshot_tiles, axis=1)
    proj_parts[seat] = split_dot(snapshots, basis_parts, 0)
    for i in range(1, inner):
        rank = plane * inner + lax.rem(seat + i, inner)
        remote(proj_parts.at[seat], proj_parts.at[seat], wide_send.at[5], wide_recv.at[5], rank).start()

    for k in range(sub_count):
        carried = green[k] - scale0 * fields0[k] - scale1 * fields1[k]
        now, vel, acc = disp_now[:, k, :], vel_now[:, k, :], acc_now[:, k, :]
        accel_new = (
            (carried - now) / (newmark_beta * time_step * time_step)
            - vel / (newmark_beta * time_step)
            - (0.5 / newmark_beta - 1.0) * acc
        )
        disp_out[:, k, :] = carried
        vel_out[:, k, :] = vel + time_step * ((1.0 - newmark_gamma) * acc + newmark_gamma * accel_new)

    pltpu.make_async_copy(
        proj_parts.at[pl.ds(0, inner - 1)], proj_parts.at[pl.ds(0, inner - 1)], wide_recv.at[5]
    ).wait()
    proj_sums[plane] = jnp.sum(proj_parts[...], axis=0)
    for i in range(1, outer):
        rank = lax.rem(plane + i, outer) * inner + seat
        remote(proj_sums.at[plane], proj_sums.at[plane], wide_send.at[7], wide_recv.at[7], rank).start()
    pltpu.make_async_copy(
        proj_sums.at[pl.ds(0, outer - 1)], proj_sums.at[pl.ds(0, outer - 1)], wide_recv.at[7]
    ).wait()
    projection = jnp.sum(proj_sums[...], axis=0)
    proj_out[...] = projection
    remainder = snapshots - split_dot(projection, basis_parts, 1)
    gram_row = jnp.zeros((8, LANES), jnp.float32)
    for shift in range(5):
        product = remainder * pltpu.roll(remainder, shift, 0)
        other = lax.rem(sublane + 8 - shift, 8)
        here = (lane == 8 * sublane + other) | ((lane == 8 * other + sublane) & (shift < 4))
        gram_row = jnp.where(here, column(product), gram_row)
    gram_parts[0, me] = jnp.sum(gram_row, axis=0, keepdims=True)
    broadcast(gram_parts, 0, 6)
    all_but_one(gram_parts, 0, wide_recv.at[6]).wait()
    gram_row = jnp.broadcast_to(jnp.sum(gram_parts[0], axis=0), (8, LANES))
    entry = {
        (i, j): jnp.broadcast_to(gram_row[:, 8 * i + j : 8 * i + j + 1], (8, LANES)) for i in range(8) for j in range(i + 1)
    }
    row_at = lax.broadcasted_iota(jnp.int32, remainder.shape, 0)
    factor = jnp.zeros((8, LANES), jnp.float32)
    for j in range(8):
        inverse_root = lax.rsqrt(entry[j, j])
        lower = {i: entry[i, j] * inverse_root for i in range(j, 8)}
        below = jnp.zeros((8, LANES), jnp.float32)
        for i in range(j, 8):
            factor = jnp.where((sublane == j) & (lane == i), lower[i], factor)
            for k in range(j + 1, i + 1):
                entry[i, k] = entry[i, k] - lower[i] * lower[k]
            if i > j:
                below = jnp.where(sublane == i, lower[i], below)
        pivot_rows = remainder[j : j + 1, :] * inverse_root[0:1, 0:1]
        remainder = jnp.where(row_at == j, pivot_rows, remainder - below[:, 0:1] * pivot_rows)
    scale_rows = math.sqrt(snapshots.shape[1] * n)
    r_out[...] = factor[:, :8] * (1.0 / scale_rows)
    cols_out[...] = remainder * scale_rows

    for copy in halos + coarse_near + [coarse_far] + edges:
        copy.wait_send()
    for at in range(3):
        all_but_one(gathered, at, wide_send.at[at]).wait()
    all_but_one(norms, 0, wide_send.at[3]).wait()
    all_but_one(incoming, 0, wide_send.at[4]).wait()
    pltpu.make_async_copy(
        proj_parts.at[pl.ds(0, inner - 1)], proj_parts.at[pl.ds(0, inner - 1)], wide_send.at[5]
    ).wait()
    pltpu.make_async_copy(
        proj_sums.at[pl.ds(0, outer - 1)], proj_sums.at[pl.ds(0, outer - 1)], wide_send.at[7]
    ).wait()
    all_but_one(gram_parts, 0, wide_send.at[6]).wait()


def solution(mesh):
    groups = mesh.shape["grp"]
    n = mesh.shape["sub"] * groups
    inner = math.gcd(n, 8)

    def shards(
        rr_inverse,
        corner_modes,
        coarse_inverse,
        inertia,
        disp_now,
        vel_now,
        acc_now,
        load_next,
        basis_rows,
        piece_owner,
    ):
        case_count, sub_count, unknowns = disp_now.shape
        rank = basis_rows.shape[1]
        local_rows = basis_rows.shape[0]
        width = (sub_count + 2) * NC
        f32 = jnp.float32
        vmem = pl.BlockSpec(memory_space=pltpu.VMEM)
        anywhere = pl.BlockSpec(memory_space=pl.ANY)
        results = (
            jax.ShapeDtypeStruct(disp_now.shape, f32),
            jax.ShapeDtypeStruct(disp_now.shape, f32),
            jax.ShapeDtypeStruct((case_count, rank), f32),
            jax.ShapeDtypeStruct((case_count, case_count), f32),
            jax.ShapeDtypeStruct((case_count, local_rows), f32),
        )
        kept = tuple(pltpu.VMEM(result.shape, f32) for result in results)
        computed = pl.pallas_call(
            functools.partial(kernel, n, groups, inner),
            out_shape=kept,
            in_specs=[anywhere] * 10,
            out_specs=(vmem,) * 5,
            scratch_shapes=[
                pltpu.SMEM(piece_owner.shape, jnp.int32),
                pltpu.SMEM(piece_owner.shape, jnp.int32),
                pltpu.VMEM(inertia.shape, f32),
                pltpu.VMEM(disp_now.shape, f32),
                pltpu.VMEM(vel_now.shape, f32),
                pltpu.VMEM(acc_now.shape, f32),
                pltpu.VMEM(load_next.shape, f32),
                pltpu.VMEM((2, width, coarse_inverse.shape[1]), jnp.bfloat16),
                pltpu.VMEM((2, width, width + 2 * NI), jnp.bfloat16),
                pltpu.VMEM((2, width, (sub_count + 1) * NI + width), jnp.bfloat16),
                pltpu.VMEM((2, width, (sub_count + 2) * NI), jnp.bfloat16),
                pltpu.VMEM((2, width, (sub_count + 1) * NI), jnp.bfloat16),
                pltpu.VMEM((2, width, sub_count * unknowns), jnp.bfloat16),
                pltpu.VMEM((2,) + basis_rows.shape, jnp.bfloat16),
                pltpu.VMEM(rr_inverse.shape, f32),
                pltpu.VMEM(corner_modes.shape, f32),
                pltpu.VMEM((width + NC, coarse_inverse.shape[1]), f32),
                pltpu.VMEM(basis_rows.shape, f32),
                pltpu.VMEM((3, 2 * NC, NI), f32),
                pltpu.VMEM((2 * NC, NI), f32),
                pltpu.VMEM((width, sub_count * unknowns), f32),
                pltpu.VMEM((width, (sub_count + 1) * NI), f32),
                pltpu.VMEM((width, (sub_count + 1) * NI), f32),
                pltpu.VMEM((width, (sub_count + 2) * NI), f32),
                pltpu.VMEM((width, (sub_count + 2) * NI), f32),
                pltpu.VMEM((3, n, case_count, width), f32),
                pltpu.VMEM((6, case_count, NI), f32),
                pltpu.VMEM((6, case_count, NI), f32),
                pltpu.VMEM((1, n, 1, LANES), f32),
                pltpu.VMEM((n, case_count, LANES), f32),
                pltpu.VMEM((n, case_count, LANES), f32),
                pltpu.VMEM((1, n, case_count, LANES), f32),
                pltpu.VMEM((inner, case_count, rank), f32),
                pltpu.VMEM((n // inner, case_count, rank), f32),
                pltpu.VMEM((1, n, 1, LANES), f32),
                pltpu.VMEM((sub_count, case_count, unknowns), f32),
                pltpu.SemaphoreType.DMA((10,)),
                pltpu.SemaphoreType.DMA((7,)),
                pltpu.SemaphoreType.DMA((7,)),
                pltpu.SemaphoreType.DMA((8,)),
                pltpu.SemaphoreType.DMA((8,)),
                pltpu.SemaphoreType.DMA((6,)),
                pltpu.SemaphoreType.DMA((6,)),
            ],
            compiler_params=pltpu.CompilerParams(collective_id=0, has_side_effects=True),
        )(
            piece_owner,
            rr_inverse,
            corner_modes,
            coarse_inverse,
            basis_rows,
            inertia,
            disp_now,
            vel_now,
            acc_now,
            load_next,
        )
        disp, vel, proj, r_factor, columns = pl.pallas_call(
            hand_over,
            out_shape=results,
            in_specs=[vmem] * 5,
            out_specs=(vmem,) * 5,
            compiler_params=pltpu.CompilerParams(vmem_limit_bytes=4 * 1024 * 1024),
        )(*computed)
        return disp, vel, proj.T, r_factor, columns

    return jax.shard_map(
        shards,
        mesh=mesh,
        in_specs=(
            P(("sub", "grp"), None, None),
            P(("sub", "grp"), None, None),
            P(("sub", "grp"), None),
            P(("sub", "grp"), None),
            P(None, ("sub", "grp"), None),
            P(None, ("sub", "grp"), None),
            P(None, ("sub", "grp"), None),
            P(None, ("sub", "grp"), None),
            P(("sub", "grp"), None),
            P(),
        ),
        out_specs=(
            P(None, ("sub", "grp"), None),
            P(None, ("sub", "grp"), None),
            P(),
            P(),
            P(None, ("sub", "grp")),
        ),
        check_vma=False,
    )
```

```python
import functools
import math

import jax
import jax.numpy as jnp
from jax import lax
from jax.experimental import pallas as pl
from jax.experimental.pallas import tpu as pltpu
from jax.sharding import PartitionSpec as P

NC = 32
NI = 128
LANES = 128

time_step = 0.5
newmark_beta = 0.25
newmark_gamma = 0.5

MESH = pl.DeviceIdType.MESH


def nn(a, b):
    return lax.dot_general(
        a, b, (((1,), (0,)), ((), ())), precision=lax.Precision.HIGHEST, preferred_element_type=jnp.float32
    )


def nt(a, b):
    return lax.dot_general(
        a, b, (((1,), (1,)), ((), ())), precision=lax.Precision.HIGHEST, preferred_element_type=jnp.float32
    )


def split(x):
    first = x.astype(jnp.bfloat16)
    return first, (x - first.astype(jnp.float32)).astype(jnp.bfloat16)


def keep_split(parts, matrix, at=0):
    for which, part in enumerate(split(matrix)):
        parts[which, at : at + matrix.shape[0]] = part


def keep_columns(parts, matrix, at=0):
    for which, part in enumerate(split(matrix)):
        parts[which, :, at : at + matrix.shape[1]] = part


def split_dot(x, parts, contracted):
    first, second = split(x)
    rows = x.shape[0]

    def product(a, b):
        return lax.dot_general(a, b, (((1,), (contracted,)), ((), ())), preferred_element_type=jnp.float32)

    large = product(jnp.concatenate([first, second], axis=0), parts[0])
    return large[:rows] + (large[rows:] + product(first, parts[1]))


def hand_over(*refs):
    half = len(refs) // 2
    for source, target in zip(refs[:half], refs[half:]):
        target[...] = source[...]


def kernel(
    n,
    groups,
    inner,
    owner_hbm,
    rr_hbm,
    modes_hbm,
    coarse_hbm,
    basis_hbm,
    inertia_hbm,
    disp_hbm,
    vel_hbm,
    acc_hbm,
    load_hbm,
    disp_out,
    vel_out,
    proj_out,
    r_out,
    cols_out,
    owner,
    inverse,
    inertia,
    disp_now,
    vel_now,
    acc_now,
    load_next,
    coarse_parts,
    early_parts,
    step_parts,
    known_parts,
    backward_parts,
    corner_parts,
    basis_parts,
    basis_across,
    rr,
    modes,
    coarse,
    basis,
    modes_next,
    modes_prev,
    corner,
    forward,
    backward,
    gathered,
    edge,
    edge_out,
    norms,
    pieces,
    outgoing,
    incoming,
    proj_parts,
    proj_sums,
    gram_parts,
    green,
    local_sem,
    const_send,
    const_recv,
    wide_send,
    wide_recv,
    edge_send,
    edge_recv,
):
    sub_count, unknowns = rr.shape[0], rr.shape[1]
    rows = sub_count * NC
    me = lax.axis_index("sub") * groups + lax.axis_index("grp")
    following = lax.rem(me + 1, n)
    earlier = lax.rem(me + n - 1, n)
    odd = lax.rem(me, 2) == 1
    partner = jnp.where(odd, earlier, following)
    outward = jnp.where(odd, following, earlier)

    def device(rank):
        return (rank // groups, lax.rem(rank, groups))

    plane, outer = me // inner, n // inner
    seat = lax.rem(me, inner)
    seats = [lax.rem(2 * inner - 1 - seat + i, inner) for i in range(inner)]
    mirrored = 2 * plane > outer - 1
    depth = jnp.where(mirrored, outer - 1 - plane, plane)
    lead = outer - 1 - 2 * depth

    def others(body):
        def step(i, carry):
            beyond = i - lead
            turn = jnp.where(lax.rem(beyond, 2) == 0, 2 * depth - beyond // 2, beyond // 2)
            at = jnp.where(i < lead, outer - 1 - i, turn)
            at = jnp.where(mirrored, outer - 1 - at, at)
            for there in seats:
                body(at * inner + there)
            return carry

        lax.fori_loop(0, outer - 1, step, 0)
        for i in range(1, inner):
            body(plane * inner + lax.rem(seat + i, inner))

    def remote(src, dst, send, recv, rank):
        return pltpu.make_async_remote_copy(
            src_ref=src, dst_ref=dst, send_sem=send, recv_sem=recv, device_id=device(rank), device_id_type=MESH
        )

    barrier = pltpu.get_barrier_semaphore()
    others(lambda rank: pl.semaphore_signal(barrier, inc=1, device_id=device(rank), device_id_type=MESH))

    load_rr = pltpu.make_async_copy(rr_hbm, rr, local_sem.at[0])
    load_modes = pltpu.make_async_copy(modes_hbm, modes, local_sem.at[1])
    load_coarse = pltpu.make_async_copy(coarse_hbm, coarse.at[pl.ds(0, rows)], local_sem.at[2])
    load_basis = pltpu.make_async_copy(basis_hbm, basis, local_sem.at[3])
    fields_in = [
        pltpu.make_async_copy(source, target, local_sem.at[4 + at])
        for at, (source, target) in enumerate(
            (
                (inertia_hbm, inertia),
                (disp_hbm, disp_now),
                (vel_hbm, vel_now),
                (acc_hbm, acc_now),
                (load_hbm, load_next),
            )
        )
    ]
    load_owner = pltpu.make_async_copy(owner_hbm, owner, local_sem.at[9])
    load_modes.start()
    for copy in fields_in:
        copy.start()
    load_owner.start()
    load_coarse.start()
    load_rr.start()
    load_basis.start()

    lane = lax.broadcasted_iota(jnp.int32, (8, LANES), 1)
    sublane = lax.broadcasted_iota(jnp.int32, (8, LANES), 0)

    def right_side(k):
        return load_next[:, k, :] + inertia[k : k + 1, :] * (
            disp_now[:, k, :]
            + time_step * vel_now[:, k, :]
            + (0.5 - newmark_beta) * time_step * time_step * acc_now[:, k, :]
        )

    for copy in fields_in:
        copy.wait()
    sides = [right_side(k) for k in range(sub_count)]

    corner[...] = jnp.zeros_like(corner)
    load_modes.wait()
    corner[0:NC, 0:unknowns] = modes[0, NC:, :]
    corner[0:NC, unknowns:] = modes[1, :NC, :]
    corner[NC : 2 * NC, unknowns:] = modes[1, NC:, :]
    corner[3 * NC :, 0:unknowns] = modes[0, :NC, :]

    def placed(tile):
        return jnp.where(odd, pltpu.roll(tile, 64, 1), tile)

    def broadcast(buffer, at, sem):
        def send(rank):
            remote(buffer.at[at, me], buffer.at[at, me], wide_send.at[sem], wide_recv.at[sem], rank).start()

        others(send)

    def all_but_one(buffer, at, sem):
        return pltpu.make_async_copy(buffer.at[at, pl.ds(0, n - 1)], buffer.at[at, pl.ds(0, n - 1)], sem)

    gathered[0, me] = placed(nt(jnp.concatenate(sides, axis=1), corner[...]))

    pl.semaphore_wait(barrier, n - 1)
    next_modes = [
        remote(modes.at[k, :, pl.ds(start, NI)], modes_next.at[at], const_send.at[at], const_recv.at[at], earlier)
        for at, (k, start) in enumerate(((0, 0), (0, unknowns - NI), (1, 0)))
    ]
    halos = next_modes + [
        remote(modes.at[1, :, pl.ds(unknowns - NI, NI)], modes_prev, const_send.at[3], const_recv.at[3], following)
    ]
    broadcast(gathered, 0, 0)
    for copy in halos:
        copy.start()
    load_coarse.wait()
    coarse_near = [
        remote(
            coarse.at[pl.ds(k * NC, NC)], coarse.at[pl.ds(slot * NC, NC)], const_send.at[4 + k], const_recv.at[4 + k], partner
        )
        for k, slot in ((0, 2), (1, 4))
    ]
    coarse_far = remote(
        coarse.at[pl.ds(NC, NC)], coarse.at[pl.ds(3 * NC, NC)], const_send.at[6], const_recv.at[6], following
    )
    for copy in coarse_near + [coarse_far]:
        copy.start()

    load_rr.wait()
    local = [nn(sides[k], rr[k]) for k in range(sub_count)]
    def facing_edge(first, last, at):
        edge_out[at] = jnp.where(odd, first, last)
        copy = remote(edge_out.at[at], edge.at[at], edge_send.at[at], edge_recv.at[at], partner)
        copy.start()
        edges.append(copy)
        return copy

    edges = []
    met = facing_edge(local[0][:, :NI], local[1][:, unknowns - NI :], 0)
    middle_known = local[0][:, unknowns - NI :] - local[1][:, :NI]
    met_middle = facing_edge(middle_known, middle_known, 5)

    load_owner.wait()

    def find(t, carry):
        at = jnp.int32(0)
        for p in range(n):
            at = jnp.where(owner[p] == t, p, at)
        inverse[t] = at
        return carry

    lax.fori_loop(0, n, find, 0)
    keep_split(corner_parts, corner[...])

    for copy in coarse_near:
        copy.wait_recv()
    keep_columns(coarse_parts, jnp.concatenate([coarse[: 3 * NC], coarse[4 * NC :]], axis=0).T)
    halos[3].wait_recv()
    first0, last0 = modes[0, :, :NI], modes[0, :, unknowns - NI :]
    first1, last1 = modes[1, :, :NI], modes[1, :, unknowns - NI :]
    before = modes_prev[...]
    empty = jnp.zeros((2 * NC, NI), jnp.float32)
    jump = {
        (-1, -2): before[:NC],
        (-1, -1): before[NC:] - first0[:NC],
        (-1, 0): -first0[NC:],
        (0, -1): last0[:NC],
        (0, 0): last0[NC:] - first1[:NC],
        (0, 1): -first1[NC:],
        (1, 0): last1[:NC],
    }

    def fill_columns(i):
        for parts, swap in ((early_parts, False), (known_parts, True)):
            blocks = []
            for ends in ((0, 0), (1, 1), (2, -2), (3, -1)):
                at_even, at_odd = [jump.get((i, end), empty[:NC]) for end in (ends[::-1] if swap else ends)]
                blocks.append(at_even if ends[0] == ends[1] else jnp.where(odd, at_odd, at_even))
            keep_columns(parts, jnp.concatenate(blocks, axis=0), (i + 1) * NI)

    fill_columns(-1)
    fill_columns(0)
    leaving = jnp.where(odd, last1, jnp.concatenate([-first0[NC:], empty[:NC]], axis=0))
    keep_columns(early_parts, jnp.concatenate([leaving, empty], axis=0), 4 * NI)
    def assemble(at):
        all_but_one(gathered, at, wide_recv.at[at]).wait()
        assembled = []
        for j in range(n // 2):
            low = jnp.where(lane < 64, gathered[at, 2 * j], gathered[at, (2 * j + 2) % n])
            high = jnp.where(lane >= (64 if at == 1 else 32), gathered[at, 2 * j + 1], gathered[at, (2 * j - 1) % n])
            assembled.append(low + high)
        return jnp.concatenate(assembled, axis=1)

    def coarse_solve(at):
        return split_dot(assemble(at), coarse_parts, 0)

    def jumps(fields, across):
        first, second = fields
        left = jnp.where(odd, across, 0.0) - first[:, :NI]
        right = second[:, unknowns - NI :] - jnp.where(odd, 0.0, across)
        return jnp.concatenate([left, first[:, unknowns - NI :] - second[:, :NI], right], axis=1)

    per_piece = unknowns // n
    width = sub_count * per_piece
    per_tile = LANES // width
    spot = lax.rem(me, per_tile)

    def piece_part(fields, which, p):
        block = p * per_piece // LANES
        inside = p * per_piece % LANES
        start = lax.rem(spot + which, per_tile) * width
        part = jnp.zeros((8, LANES), jnp.float32)
        for k in range(sub_count):
            target = start + k * per_piece
            rolled = pltpu.roll(
                fields[k][:, block * LANES : (block + 1) * LANES], lax.rem(target + LANES - inside, LANES), 1
            )
            part = jnp.where((lane >= target) & (lane < target + per_piece), rolled, part)
        return part

    def outer_half(vector, at):
        slot = 2 * at - 1
        edge_out[slot] = vector
        copy = remote(edge_out.at[slot], edge.at[slot], edge_send.at[slot], edge_recv.at[slot], outward)
        copy.start()
        edges.append(copy)
        return copy

    def send_terms(terms, at):
        gathered[at, me] = placed(terms)
        broadcast(gathered, at, at)

    def outermost(vector):
        return jnp.where(odd, vector[:, 2 * NI : 3 * NI], vector[:, :NI])

    def facing_field(vector, at):
        left, middle, right = vector[:, :NI], vector[:, NI : 2 * NI], vector[:, 2 * NI :]
        near = rr.at[jnp.where(odd, 0, 1)]
        facing = nn(jnp.where(odd, -left, -middle), near[:NI, :]) + nn(
            jnp.where(odd, middle, right), near[unknowns - NI :, :]
        )
        return facing_edge(facing[:, :NI], facing[:, unknowns - NI :], 2 * at), facing

    met.wait_recv()
    known = jumps(local, edge[0])
    met_middle.wait_recv()
    known_wide = jnp.concatenate([known, jnp.where(odd, 0.0, edge[5])], axis=1)
    assembled = assemble(0)
    solved = split_dot(assembled, coarse_parts, 0)
    for copy in next_modes:
        copy.wait_recv()
    after, after_last, after_first1 = modes_next[0], modes_next[1], modes_next[2]
    jump.update(
        {
            (1, 1): last1[NC:] - after[:NC],
            (1, 2): -after[NC:],
            (2, 1): after_last[:NC],
            (2, 2): after_last[NC:] - after_first1[:NC],
            (2, 3): -after_first1[NC:],
        }
    )
    fill_columns(1)
    fill_columns(2)
    keep_columns(early_parts, jnp.concatenate([empty[:NC], jnp.where(odd, -after[:NC], 0.0), empty], axis=0), 5 * NI)
    early = split_dot(solved, early_parts, 0)
    sent0 = outer_half(outermost(known) + early[:, 4 * NI : 5 * NI], 1)
    send_terms(split_dot(known_wide + early[:, : 4 * NI], known_parts, 1), 1)
    forward[...] = jnp.zeros_like(forward)
    forward[0:NC, 0:NI] = -first0[NC:]
    forward[0:NC, NI : 2 * NI] = last0[NC:] - first1[:NC]
    forward[0:NC, 2 * NI :] = last1[:NC]
    forward[NC : 2 * NC, NI : 2 * NI] = -first1[NC:]
    forward[NC : 2 * NC, 2 * NI :] = last1[NC:] - jnp.where(odd, 0.0, after[:NC])
    forward[2 * NC : 3 * NC, 0:NI] = jnp.where(odd, before[:NC], 0.0)
    forward[2 * NC : 3 * NC, 2 * NI :] = jnp.where(odd, 0.0, -after[NC:])
    forward[3 * NC :, 0:NI] = jnp.where(odd, before[NC:], 0.0) - first0[:NC]
    forward[3 * NC :, NI : 2 * NI] = last0[:NC]
    backward[...] = jnp.zeros_like(backward)
    backward[0:NC, :] = forward[0:NC, :]
    backward[NC : 2 * NC, NI : 2 * NI] = -first1[NC:]
    backward[NC : 2 * NC, 2 * NI :] = last1[NC:] - after[:NC]
    backward[2 * NC : 3 * NC, 0:NI] = jnp.where(odd, 0.0, before[:NC])
    backward[2 * NC : 3 * NC, 2 * NI :] = jnp.where(odd, -after[NC:], 0.0)
    backward[3 * NC :, 0:NI] = jnp.where(odd, 0.0, before[NC:] - first0[:NC])
    backward[3 * NC :, NI : 2 * NI] = last0[:NC]

    keep_split(step_parts, jnp.concatenate([forward[...], nt(forward[...], backward[...])], axis=1))
    keep_split(backward_parts, backward[...])
    extra = early[:, 5 * NI :]
    coarse_far.wait_recv()
    keep_columns(coarse_parts, coarse[: 4 * NC].T)
    solved = jnp.concatenate([solved[:, : 3 * NC], split_dot(assembled, coarse_parts, 0)[:, 3 * NC :]], axis=1)
    vector0 = known + split_dot(solved, step_parts, 0)[:, : 3 * NI]
    met0, facing0 = facing_field(vector0, 1)

    def whole(vector, copy, at, extra=0.0):
        copy.wait_recv()
        other = edge[2 * at - 1] + extra
        return jnp.concatenate(
            [
                vector[:, :NI] + jnp.where(odd, 0.0, other),
                vector[:, NI : 2 * NI],
                vector[:, 2 * NI :] + jnp.where(odd, other, 0.0),
            ],
            axis=1,
        )

    def end_image(full, met, facing, at):
        left, middle, right = full[:, :NI], full[:, NI : 2 * NI], full[:, 2 * NI :]
        far = rr.at[jnp.where(odd, 1, 0)]
        outer_field = nn(jnp.where(odd, -middle, -left), far[:NI, :]) + nn(
            jnp.where(odd, right, middle), far[unknowns - NI :, :]
        )
        inside = [jnp.where(odd, facing, outer_field), jnp.where(odd, outer_field, facing)]
        met.wait_recv()
        known = jumps(inside, edge[2 * at])
        carried = split_dot(known, backward_parts, 1)
        return inside, known, carried, coarse_solve(at)

    def counted(vector):
        return jnp.concatenate([jnp.where(odd, 0.0, vector[:, :NI]), vector[:, NI:]], axis=1)

    def with_corners(inside, values):
        added = split_dot(values, corner_parts, 0)
        return [inside[k] + added[:, k * unknowns : (k + 1) * unknowns] for k in range(sub_count)]

    def column(values):
        return jnp.sum(values, axis=1, keepdims=True)

    first_fields = with_corners(local, solved)
    for k in range(sub_count):
        green[k] = first_fields[k]
    for p in range(n):
        pieces[p] = piece_part(first_fields, 0, p)
    full0 = whole(vector0, sent0, 1, extra)
    inside0, known, carried, values0 = end_image(full0, met0, facing0, 1)

    step = split_dot(values0, step_parts, 0)
    vector1 = known + step[:, : 3 * NI]
    sent1 = outer_half(outermost(vector1), 2)
    send_terms(carried + step[:, 3 * NI :], 2)
    norm_row = jnp.where(lane == sublane, column(full0 * counted(vector0)), 0.0) + jnp.where(
        lane == sublane + 8, column(full0 * counted(vector1)), 0.0
    )
    norms[0, me] = jnp.sum(norm_row, axis=0, keepdims=True)
    broadcast(norms, 0, 3)
    met1, facing1 = facing_field(vector1, 2)
    fields0 = with_corners(inside0, values0)
    for p in range(n):
        pieces[p] = pieces[p] + piece_part(fields0, 1, p)
    load_basis.wait()
    keep_split(basis_parts, basis[...])
    full1 = whole(vector1, sent1, 2)
    weighed0, weighed1 = [
        split_dot(counted(full), step_parts.at[:, :, pl.ds(0, 3 * NI)], 1) for full in (full0, full1)
    ]
    inside1, known, carried, values1 = end_image(full1, met1, facing1, 2)
    fields1 = with_corners(inside1, values1)

    all_but_one(norms, 0, wide_recv.at[3]).wait()
    totals = jnp.broadcast_to(jnp.sum(norms[0], axis=0), (8, LANES))
    norm0, curve0 = [column(jnp.where(lane == sublane + 8 * which, totals, 0.0)) for which in range(2)]
    alpha0 = norm0 / curve0
    residual = counted(full0 - alpha0 * full1)
    free = lax.rem(spot + 3, per_tile) * width + per_piece
    extra = (
        jnp.where(lane == free, column(residual * (vector0 - alpha0 * vector1)), 0.0)
        + jnp.where(
            lane == free + 1,
            column(residual * (vector1 - alpha0 * known))
            - alpha0 * column((weighed0 - alpha0 * weighed1) * values1),
            0.0,
        )
        + jnp.where(lane == free + 2, column(residual * vector1), 0.0)
    )
    for p in range(n):
        pieces[p] = pieces[p] + piece_part(fields1, 2, p) + extra
    for t in range(n):
        outgoing[t] = pieces[inverse[t]]

    def send_piece(rank):
        remote(outgoing.at[rank], incoming.at[0, me], wide_send.at[4], wide_recv.at[4], rank).start()

    others(send_piece)
    incoming[0, me] = outgoing[me]
    keep_columns(basis_across, basis[...].T)
    all_but_one(incoming, 0, wide_recv.at[4]).wait()
    gathered_sums = jnp.zeros((8, LANES), jnp.float32)
    for i in range(per_tile):
        total = incoming[0, i]
        for j in range(1, n // per_tile):
            total = total + incoming[0, j * per_tile + i]
        at = (i + 3) % per_tile * width + per_piece
        gathered_sums = jnp.where((lane >= at) & (lane < at + 3), total, gathered_sums)
    norm1, curve_rr, curve_rp = [
        column(jnp.where(lax.rem(lane, width) == per_piece + which, gathered_sums, 0.0)) for which in range(3)
    ]
    beta = norm1 / norm0
    curve1 = curve_rr + 2.0 * beta * curve_rp + beta * beta * curve0
    alpha1 = norm1 / curve1
    scale0 = alpha0 + alpha1 * (1.0 + beta)
    scale1 = -alpha1 * alpha0

    snapshot_tiles = []
    for j in range(n // per_tile):
        total = jnp.zeros((8, LANES), jnp.float32)
        for which, factor in enumerate((1.0, -scale0, -scale1)):
            tile = incoming[0, j * per_tile]
            for i in range(1, per_tile):
                block = (i + which) % per_tile
                inside = (lane >= block * width) & (lane < (block + 1) * width)
                tile = jnp.where(inside, incoming[0, j * per_tile + i], tile)
            if which:
                tile = pltpu.roll(tile, LANES - which * width, 1)
            total = total + factor * tile
        snapshot_tiles.append(total)
    snapshots = jnp.concatenate(snapshot_tiles, axis=1)
    proj_parts[seat] = split_dot(snapshots, basis_parts, 0)
    for i in range(1, inner):
        rank = plane * inner + lax.rem(seat + i, inner)
        remote(proj_parts.at[seat], proj_parts.at[seat], wide_send.at[5], wide_recv.at[5], rank).start()

    for copy in halos + coarse_near + [coarse_far] + edges:
        copy.wait_send()
    for at in range(3):
        all_but_one(gathered, at, wide_send.at[at]).wait()
    all_but_one(norms, 0, wide_send.at[3]).wait()
    all_but_one(incoming, 0, wide_send.at[4]).wait()

    for k in range(sub_count):
        carried = green[k] - scale0 * fields0[k] - scale1 * fields1[k]
        now, vel, acc = disp_now[:, k, :], vel_now[:, k, :], acc_now[:, k, :]
        accel_new = (
            (carried - now) / (newmark_beta * time_step * time_step)
            - vel / (newmark_beta * time_step)
            - (0.5 / newmark_beta - 1.0) * acc
        )
        disp_out[:, k, :] = carried
        vel_out[:, k, :] = vel + time_step * ((1.0 - newmark_gamma) * acc + newmark_gamma * accel_new)

    pltpu.make_async_copy(
        proj_parts.at[pl.ds(0, inner - 1)], proj_parts.at[pl.ds(0, inner - 1)], wide_recv.at[5]
    ).wait()
    proj_sums[plane] = jnp.sum(proj_parts[...], axis=0)
    for i in range(1, outer):
        rank = lax.rem(plane + i, outer) * inner + seat
        remote(proj_sums.at[plane], proj_sums.at[plane], wide_send.at[7], wide_recv.at[7], rank).start()
    pltpu.make_async_copy(
        proj_sums.at[pl.ds(0, outer - 1)], proj_sums.at[pl.ds(0, outer - 1)], wide_recv.at[7]
    ).wait()
    projection = jnp.sum(proj_sums[...], axis=0)
    proj_out[...] = projection
    remainder = snapshots - split_dot(projection, basis_across, 0)
    gram_row = jnp.zeros((8, LANES), jnp.float32)
    for shift in range(5):
        product = remainder * pltpu.roll(remainder, shift, 0)
        other = lax.rem(sublane + 8 - shift, 8)
        here = (lane == 8 * sublane + other) | ((lane == 8 * other + sublane) & (shift < 4))
        gram_row = jnp.where(here, column(product), gram_row)
    gram_parts[0, me] = jnp.sum(gram_row, axis=0, keepdims=True)
    broadcast(gram_parts, 0, 6)
    pltpu.make_async_copy(
        proj_parts.at[pl.ds(0, inner - 1)], proj_parts.at[pl.ds(0, inner - 1)], wide_send.at[5]
    ).wait()
    pltpu.make_async_copy(
        proj_sums.at[pl.ds(0, outer - 1)], proj_sums.at[pl.ds(0, outer - 1)], wide_send.at[7]
    ).wait()
    all_but_one(gram_parts, 0, wide_recv.at[6]).wait()
    gram_row = jnp.broadcast_to(jnp.sum(gram_parts[0], axis=0), (8, LANES))
    entry = {
        (i, j): jnp.broadcast_to(gram_row[:, 8 * i + j : 8 * i + j + 1], (8, LANES)) for i in range(8) for j in range(i + 1)
    }
    row_at = lax.broadcasted_iota(jnp.int32, remainder.shape, 0)
    factor = jnp.zeros((8, LANES), jnp.float32)
    for j in range(8):
        inverse_root = lax.rsqrt(entry[j, j])
        lower = {i: entry[i, j] * inverse_root for i in range(j, 8)}
        below = jnp.zeros((8, LANES), jnp.float32)
        for i in range(j, 8):
            factor = jnp.where((sublane == j) & (lane == i), lower[i], factor)
            for k in range(j + 1, i + 1):
                entry[i, k] = entry[i, k] - lower[i] * lower[k]
            if i > j:
                below = jnp.where(sublane == i, lower[i], below)
        pivot_rows = remainder[j : j + 1, :] * inverse_root[0:1, 0:1]
        remainder = jnp.where(row_at == j, pivot_rows, remainder - below[:, 0:1] * pivot_rows)
    scale_rows = math.sqrt(snapshots.shape[1] * n)
    r_out[...] = factor[:, :8] * (1.0 / scale_rows)
    cols_out[...] = remainder * scale_rows

    all_but_one(gram_parts, 0, wide_send.at[6]).wait()


def solution(mesh):
    groups = mesh.shape["grp"]
    n = mesh.shape["sub"] * groups
    inner = math.gcd(n, 8)

    def shards(
        rr_inverse,
        corner_modes,
        coarse_inverse,
        inertia,
        disp_now,
        vel_now,
        acc_now,
        load_next,
        basis_rows,
        piece_owner,
    ):
        case_count, sub_count, unknowns = disp_now.shape
        rank = basis_rows.shape[1]
        local_rows = basis_rows.shape[0]
        width = (sub_count + 2) * NC
        f32 = jnp.float32
        vmem = pl.BlockSpec(memory_space=pltpu.VMEM)
        anywhere = pl.BlockSpec(memory_space=pl.ANY)
        results = (
            jax.ShapeDtypeStruct(disp_now.shape, f32),
            jax.ShapeDtypeStruct(disp_now.shape, f32),
            jax.ShapeDtypeStruct((case_count, rank), f32),
            jax.ShapeDtypeStruct((case_count, case_count), f32),
            jax.ShapeDtypeStruct((case_count, local_rows), f32),
        )
        kept = tuple(pltpu.VMEM(result.shape, f32) for result in results)
        computed = pl.pallas_call(
            functools.partial(kernel, n, groups, inner),
            out_shape=kept,
            in_specs=[anywhere] * 10,
            out_specs=(vmem,) * 5,
            scratch_shapes=[
                pltpu.SMEM(piece_owner.shape, jnp.int32),
                pltpu.SMEM(piece_owner.shape, jnp.int32),
                pltpu.VMEM(inertia.shape, f32),
                pltpu.VMEM(disp_now.shape, f32),
                pltpu.VMEM(vel_now.shape, f32),
                pltpu.VMEM(acc_now.shape, f32),
                pltpu.VMEM(load_next.shape, f32),
                pltpu.VMEM((2, coarse_inverse.shape[1], width), jnp.bfloat16),
                pltpu.VMEM((2, width, (sub_count + 4) * NI), jnp.bfloat16),
                pltpu.VMEM((2, width, (sub_count + 1) * NI + width), jnp.bfloat16),
                pltpu.VMEM((2, width, (sub_count + 2) * NI), jnp.bfloat16),
                pltpu.VMEM((2, width, (sub_count + 1) * NI), jnp.bfloat16),
                pltpu.VMEM((2, width, sub_count * unknowns), jnp.bfloat16),
                pltpu.VMEM((2,) + basis_rows.shape, jnp.bfloat16),
                pltpu.VMEM((2,) + basis_rows.shape[::-1], jnp.bfloat16),
                pltpu.VMEM(rr_inverse.shape, f32),
                pltpu.VMEM(corner_modes.shape, f32),
                pltpu.VMEM((width + NC, coarse_inverse.shape[1]), f32),
                pltpu.VMEM(basis_rows.shape, f32),
                pltpu.VMEM((3, 2 * NC, NI), f32),
                pltpu.VMEM((2 * NC, NI), f32),
                pltpu.VMEM((width, sub_count * unknowns), f32),
                pltpu.VMEM((width, (sub_count + 1) * NI), f32),
                pltpu.VMEM((width, (sub_count + 1) * NI), f32),
                pltpu.VMEM((3, n, case_count, width), f32),
                pltpu.VMEM((6, case_count, NI), f32),
                pltpu.VMEM((6, case_count, NI), f32),
                pltpu.VMEM((1, n, 1, LANES), f32),
                pltpu.VMEM((n, case_count, LANES), f32),
                pltpu.VMEM((n, case_count, LANES), f32),
                pltpu.VMEM((1, n, case_count, LANES), f32),
                pltpu.VMEM((inner, case_count, rank), f32),
                pltpu.VMEM((n // inner, case_count, rank), f32),
                pltpu.VMEM((1, n, 1, LANES), f32),
                pltpu.VMEM((sub_count, case_count, unknowns), f32),
                pltpu.SemaphoreType.DMA((10,)),
                pltpu.SemaphoreType.DMA((7,)),
                pltpu.SemaphoreType.DMA((7,)),
                pltpu.SemaphoreType.DMA((8,)),
                pltpu.SemaphoreType.DMA((8,)),
                pltpu.SemaphoreType.DMA((6,)),
                pltpu.SemaphoreType.DMA((6,)),
            ],
            compiler_params=pltpu.CompilerParams(collective_id=0, has_side_effects=True),
        )(
            piece_owner,
            rr_inverse,
            corner_modes,
            coarse_inverse,
            basis_rows,
            inertia,
            disp_now,
            vel_now,
            acc_now,
            load_next,
        )
        disp, vel, proj, r_factor, columns = pl.pallas_call(
            hand_over,
            out_shape=results,
            in_specs=[vmem] * 5,
            out_specs=(vmem,) * 5,
            compiler_params=pltpu.CompilerParams(vmem_limit_bytes=4 * 1024 * 1024),
        )(*computed)
        return disp, vel, proj.T, r_factor, columns

    return jax.shard_map(
        shards,
        mesh=mesh,
        in_specs=(
            P(("sub", "grp"), None, None),
            P(("sub", "grp"), None, None),
            P(("sub", "grp"), None),
            P(("sub", "grp"), None),
            P(None, ("sub", "grp"), None),
            P(None, ("sub", "grp"), None),
            P(None, ("sub", "grp"), None),
            P(None, ("sub", "grp"), None),
            P(("sub", "grp"), None),
            P(),
        ),
        out_specs=(
            P(None, ("sub", "grp"), None),
            P(None, ("sub", "grp"), None),
            P(),
            P(),
            P(None, ("sub", "grp")),
        ),
        check_vma=False,
    )
```

```python
import functools
import math

import jax
import jax.numpy as jnp
from jax import lax
from jax.experimental import pallas as pl
from jax.experimental.pallas import tpu as pltpu
from jax.sharding import PartitionSpec as P

NC = 32
NI = 128
LANES = 128

time_step = 0.5
newmark_beta = 0.25
newmark_gamma = 0.5

MESH = pl.DeviceIdType.MESH


def nn(a, b):
    return lax.dot_general(
        a, b, (((1,), (0,)), ((), ())), precision=lax.Precision.HIGHEST, preferred_element_type=jnp.float32
    )


def nt(a, b):
    return lax.dot_general(
        a, b, (((1,), (1,)), ((), ())), precision=lax.Precision.HIGHEST, preferred_element_type=jnp.float32
    )


def split(x):
    first = x.astype(jnp.bfloat16)
    return first, (x - first.astype(jnp.float32)).astype(jnp.bfloat16)


def keep_split(parts, matrix, at=0):
    for which, part in enumerate(split(matrix)):
        parts[which, at : at + matrix.shape[0]] = part


def keep_columns(parts, matrix, at=0):
    for which, part in enumerate(split(matrix)):
        parts[which, :, at : at + matrix.shape[1]] = part


def split_dot(x, parts, contracted):
    first, second = split(x)
    rows = x.shape[0]

    def product(a, b):
        return lax.dot_general(a, b, (((1,), (contracted,)), ((), ())), preferred_element_type=jnp.float32)

    large = product(jnp.concatenate([first, second], axis=0), parts[0])
    return large[:rows] + (large[rows:] + product(first, parts[1]))


def hand_over(*refs):
    half = len(refs) // 2
    for source, target in zip(refs[:half], refs[half:]):
        target[...] = source[...]


def kernel(
    n,
    groups,
    inner,
    owner_hbm,
    rr_hbm,
    modes_hbm,
    coarse_hbm,
    basis_hbm,
    inertia_hbm,
    disp_hbm,
    vel_hbm,
    acc_hbm,
    load_hbm,
    disp_out,
    vel_out,
    proj_out,
    r_out,
    cols_out,
    owner,
    inverse,
    inertia,
    disp_now,
    vel_now,
    acc_now,
    load_next,
    coarse_parts,
    early_parts,
    step_parts,
    known_parts,
    backward_parts,
    corner_parts,
    basis_parts,
    basis_across,
    rr,
    modes,
    coarse,
    basis,
    modes_next,
    modes_prev,
    corner,
    forward,
    backward,
    gathered,
    edge,
    edge_out,
    norms,
    pieces,
    outgoing,
    incoming,
    proj_parts,
    proj_sums,
    gram_parts,
    green,
    local_sem,
    const_send,
    const_recv,
    wide_send,
    wide_recv,
    edge_send,
    edge_recv,
):
    sub_count, unknowns = rr.shape[0], rr.shape[1]
    rows = sub_count * NC
    me = lax.axis_index("sub") * groups + lax.axis_index("grp")
    following = lax.rem(me + 1, n)
    earlier = lax.rem(me + n - 1, n)
    odd = lax.rem(me, 2) == 1
    partner = jnp.where(odd, earlier, following)
    outward = jnp.where(odd, following, earlier)

    def device(rank):
        return (rank // groups, lax.rem(rank, groups))

    plane, outer = me // inner, n // inner
    seat = lax.rem(me, inner)
    bits = inner.bit_length() - 1

    def flipped(mask):
        parts = [lax.rem(seat // 2**bit + mask // 2**bit, 2) * 2**bit for bit in range(bits)]
        return sum(parts[1:], parts[0]) if parts else seat

    masks = sorted(range(inner), key=lambda mask: (-mask.bit_count(), -mask))
    seats = [flipped(mask) for mask in masks]
    mirrored = 2 * plane > outer - 1
    depth = jnp.where(mirrored, outer - 1 - plane, plane)
    lead = outer - 1 - 2 * depth

    def others(body):
        def step(i, carry):
            beyond = i - lead
            turn = jnp.where(lax.rem(beyond, 2) == 0, 2 * depth - beyond // 2, beyond // 2)
            at = jnp.where(i < lead, outer - 1 - i, turn)
            at = jnp.where(mirrored, outer - 1 - at, at)
            for there in seats:
                body(at * inner + there)
            return carry

        lax.fori_loop(0, outer - 1, step, 0)
        for there in seats[:-1]:
            body(plane * inner + there)

    def remote(src, dst, send, recv, rank):
        return pltpu.make_async_remote_copy(
            src_ref=src, dst_ref=dst, send_sem=send, recv_sem=recv, device_id=device(rank), device_id_type=MESH
        )

    barrier = pltpu.get_barrier_semaphore()
    others(lambda rank: pl.semaphore_signal(barrier, inc=1, device_id=device(rank), device_id_type=MESH))

    load_rr = pltpu.make_async_copy(rr_hbm, rr, local_sem.at[0])
    load_modes = pltpu.make_async_copy(modes_hbm, modes, local_sem.at[1])
    load_coarse = pltpu.make_async_copy(coarse_hbm, coarse.at[pl.ds(0, rows)], local_sem.at[2])
    load_basis = pltpu.make_async_copy(basis_hbm, basis, local_sem.at[3])
    fields_in = [
        pltpu.make_async_copy(source, target, local_sem.at[4 + at])
        for at, (source, target) in enumerate(
            (
                (inertia_hbm, inertia),
                (disp_hbm, disp_now),
                (vel_hbm, vel_now),
                (acc_hbm, acc_now),
                (load_hbm, load_next),
            )
        )
    ]
    load_owner = pltpu.make_async_copy(owner_hbm, owner, local_sem.at[9])
    load_modes.start()
    for copy in fields_in:
        copy.start()
    load_owner.start()
    load_coarse.start()
    load_rr.start()
    load_basis.start()

    lane = lax.broadcasted_iota(jnp.int32, (8, LANES), 1)
    sublane = lax.broadcasted_iota(jnp.int32, (8, LANES), 0)

    def right_side(k):
        return load_next[:, k, :] + inertia[k : k + 1, :] * (
            disp_now[:, k, :]
            + time_step * vel_now[:, k, :]
            + (0.5 - newmark_beta) * time_step * time_step * acc_now[:, k, :]
        )

    for copy in fields_in:
        copy.wait()
    sides = [right_side(k) for k in range(sub_count)]

    corner[...] = jnp.zeros_like(corner)
    load_modes.wait()
    corner[0:NC, 0:unknowns] = modes[0, NC:, :]
    corner[0:NC, unknowns:] = modes[1, :NC, :]
    corner[NC : 2 * NC, unknowns:] = modes[1, NC:, :]
    corner[3 * NC :, 0:unknowns] = modes[0, :NC, :]

    def placed(tile):
        return jnp.where(odd, pltpu.roll(tile, 64, 1), tile)

    def broadcast(buffer, at, sem):
        def send(rank):
            remote(buffer.at[at, me], buffer.at[at, me], wide_send.at[sem], wide_recv.at[sem], rank).start()

        others(send)

    def all_but_one(buffer, at, sem):
        return pltpu.make_async_copy(buffer.at[at, pl.ds(0, n - 1)], buffer.at[at, pl.ds(0, n - 1)], sem)

    gathered[0, me] = placed(nt(jnp.concatenate(sides, axis=1), corner[...]))

    pl.semaphore_wait(barrier, n - 1)
    next_modes = [
        remote(modes.at[k, :, pl.ds(start, NI)], modes_next.at[at], const_send.at[at], const_recv.at[at], earlier)
        for at, (k, start) in enumerate(((0, 0), (0, unknowns - NI), (1, 0)))
    ]
    halos = next_modes + [
        remote(modes.at[1, :, pl.ds(unknowns - NI, NI)], modes_prev, const_send.at[3], const_recv.at[3], following)
    ]
    broadcast(gathered, 0, 0)
    for copy in halos:
        copy.start()
    load_coarse.wait()
    coarse_near = [
        remote(
            coarse.at[pl.ds(k * NC, NC)], coarse.at[pl.ds(slot * NC, NC)], const_send.at[4 + k], const_recv.at[4 + k], partner
        )
        for k, slot in ((0, 2), (1, 4))
    ]
    coarse_far = remote(
        coarse.at[pl.ds(NC, NC)], coarse.at[pl.ds(3 * NC, NC)], const_send.at[6], const_recv.at[6], following
    )
    for copy in coarse_near + [coarse_far]:
        copy.start()

    load_rr.wait()
    local = [nn(sides[k], rr[k]) for k in range(sub_count)]
    def facing_edge(first, last, at):
        edge_out[at] = jnp.where(odd, first, last)
        copy = remote(edge_out.at[at], edge.at[at], edge_send.at[at], edge_recv.at[at], partner)
        copy.start()
        edges.append(copy)
        return copy

    edges = []
    met = facing_edge(local[0][:, :NI], local[1][:, unknowns - NI :], 0)
    middle_known = local[0][:, unknowns - NI :] - local[1][:, :NI]
    met_middle = facing_edge(middle_known, middle_known, 5)

    load_owner.wait()

    def find(t, carry):
        at = jnp.int32(0)
        for p in range(n):
            at = jnp.where(owner[p] == t, p, at)
        inverse[t] = at
        return carry

    lax.fori_loop(0, n, find, 0)
    keep_split(corner_parts, corner[...])

    for copy in coarse_near:
        copy.wait_recv()
    keep_columns(coarse_parts, jnp.concatenate([coarse[: 3 * NC], coarse[4 * NC :]], axis=0).T)
    halos[3].wait_recv()
    first0, last0 = modes[0, :, :NI], modes[0, :, unknowns - NI :]
    first1, last1 = modes[1, :, :NI], modes[1, :, unknowns - NI :]
    before = modes_prev[...]
    empty = jnp.zeros((2 * NC, NI), jnp.float32)
    jump = {
        (-1, -2): before[:NC],
        (-1, -1): before[NC:] - first0[:NC],
        (-1, 0): -first0[NC:],
        (0, -1): last0[:NC],
        (0, 0): last0[NC:] - first1[:NC],
        (0, 1): -first1[NC:],
        (1, 0): last1[:NC],
    }

    def fill_columns(i):
        for parts, swap in ((early_parts, False), (known_parts, True)):
            blocks = []
            for ends in ((0, 0), (1, 1), (2, -2), (3, -1)):
                at_even, at_odd = [jump.get((i, end), empty[:NC]) for end in (ends[::-1] if swap else ends)]
                blocks.append(at_even if ends[0] == ends[1] else jnp.where(odd, at_odd, at_even))
            keep_columns(parts, jnp.concatenate(blocks, axis=0), (i + 1) * NI)

    fill_columns(-1)
    fill_columns(0)
    leaving = jnp.where(odd, last1, jnp.concatenate([-first0[NC:], empty[:NC]], axis=0))
    keep_columns(early_parts, jnp.concatenate([leaving, empty], axis=0), 4 * NI)
    def assemble(at):
        all_but_one(gathered, at, wide_recv.at[at]).wait()
        assembled = []
        for j in range(n // 2):
            low = jnp.where(lane < 64, gathered[at, 2 * j], gathered[at, (2 * j + 2) % n])
            high = jnp.where(lane >= (64 if at == 1 else 32), gathered[at, 2 * j + 1], gathered[at, (2 * j - 1) % n])
            assembled.append(low + high)
        return jnp.concatenate(assembled, axis=1)

    def coarse_solve(at):
        return split_dot(assemble(at), coarse_parts, 0)

    def jumps(fields, across):
        first, second = fields
        left = jnp.where(odd, across, 0.0) - first[:, :NI]
        right = second[:, unknowns - NI :] - jnp.where(odd, 0.0, across)
        return jnp.concatenate([left, first[:, unknowns - NI :] - second[:, :NI], right], axis=1)

    per_piece = unknowns // n
    width = sub_count * per_piece
    per_tile = LANES // width
    spot = lax.rem(me, per_tile)

    def piece_part(fields, which, p):
        block = p * per_piece // LANES
        inside = p * per_piece % LANES
        start = lax.rem(spot + which, per_tile) * width
        part = jnp.zeros((8, LANES), jnp.float32)
        for k in range(sub_count):
            target = start + k * per_piece
            rolled = pltpu.roll(
                fields[k][:, block * LANES : (block + 1) * LANES], lax.rem(target + LANES - inside, LANES), 1
            )
            part = jnp.where((lane >= target) & (lane < target + per_piece), rolled, part)
        return part

    def outer_half(vector, at):
        slot = 2 * at - 1
        edge_out[slot] = vector
        copy = remote(edge_out.at[slot], edge.at[slot], edge_send.at[slot], edge_recv.at[slot], outward)
        copy.start()
        edges.append(copy)
        return copy

    def send_terms(terms, at):
        gathered[at, me] = placed(terms)
        broadcast(gathered, at, at)

    def outermost(vector):
        return jnp.where(odd, vector[:, 2 * NI : 3 * NI], vector[:, :NI])

    def facing_field(vector, at):
        left, middle, right = vector[:, :NI], vector[:, NI : 2 * NI], vector[:, 2 * NI :]
        near = rr.at[jnp.where(odd, 0, 1)]
        facing = nn(jnp.where(odd, -left, -middle), near[:NI, :]) + nn(
            jnp.where(odd, middle, right), near[unknowns - NI :, :]
        )
        return facing_edge(facing[:, :NI], facing[:, unknowns - NI :], 2 * at), facing

    met.wait_recv()
    known = jumps(local, edge[0])
    met_middle.wait_recv()
    known_wide = jnp.concatenate([known, jnp.where(odd, 0.0, edge[5])], axis=1)
    assembled = assemble(0)
    solved = split_dot(assembled, coarse_parts, 0)
    for copy in next_modes:
        copy.wait_recv()
    after, after_last, after_first1 = modes_next[0], modes_next[1], modes_next[2]
    jump.update(
        {
            (1, 1): last1[NC:] - after[:NC],
            (1, 2): -after[NC:],
            (2, 1): after_last[:NC],
            (2, 2): after_last[NC:] - after_first1[:NC],
            (2, 3): -after_first1[NC:],
        }
    )
    fill_columns(1)
    fill_columns(2)
    keep_columns(early_parts, jnp.concatenate([empty[:NC], jnp.where(odd, -after[:NC], 0.0), empty], axis=0), 5 * NI)
    early = split_dot(solved, early_parts, 0)
    sent0 = outer_half(outermost(known) + early[:, 4 * NI : 5 * NI], 1)
    send_terms(split_dot(known_wide + early[:, : 4 * NI], known_parts, 1), 1)
    forward[...] = jnp.zeros_like(forward)
    forward[0:NC, 0:NI] = -first0[NC:]
    forward[0:NC, NI : 2 * NI] = last0[NC:] - first1[:NC]
    forward[0:NC, 2 * NI :] = last1[:NC]
    forward[NC : 2 * NC, NI : 2 * NI] = -first1[NC:]
    forward[NC : 2 * NC, 2 * NI :] = last1[NC:] - jnp.where(odd, 0.0, after[:NC])
    forward[2 * NC : 3 * NC, 0:NI] = jnp.where(odd, before[:NC], 0.0)
    forward[2 * NC : 3 * NC, 2 * NI :] = jnp.where(odd, 0.0, -after[NC:])
    forward[3 * NC :, 0:NI] = jnp.where(odd, before[NC:], 0.0) - first0[:NC]
    forward[3 * NC :, NI : 2 * NI] = last0[:NC]
    backward[...] = jnp.zeros_like(backward)
    backward[0:NC, :] = forward[0:NC, :]
    backward[NC : 2 * NC, NI : 2 * NI] = -first1[NC:]
    backward[NC : 2 * NC, 2 * NI :] = last1[NC:] - after[:NC]
    backward[2 * NC : 3 * NC, 0:NI] = jnp.where(odd, 0.0, before[:NC])
    backward[2 * NC : 3 * NC, 2 * NI :] = jnp.where(odd, -after[NC:], 0.0)
    backward[3 * NC :, 0:NI] = jnp.where(odd, 0.0, before[NC:] - first0[:NC])
    backward[3 * NC :, NI : 2 * NI] = last0[:NC]

    keep_split(step_parts, jnp.concatenate([forward[...], nt(forward[...], backward[...])], axis=1))
    keep_split(backward_parts, backward[...])
    extra = early[:, 5 * NI :]
    coarse_far.wait_recv()
    keep_columns(coarse_parts, coarse[: 4 * NC].T)
    solved = jnp.concatenate([solved[:, : 3 * NC], split_dot(assembled, coarse_parts, 0)[:, 3 * NC :]], axis=1)
    vector0 = known + split_dot(solved, step_parts, 0)[:, : 3 * NI]
    met0, facing0 = facing_field(vector0, 1)

    def whole(vector, copy, at, extra=0.0):
        copy.wait_recv()
        other = edge[2 * at - 1] + extra
        return jnp.concatenate(
            [
                vector[:, :NI] + jnp.where(odd, 0.0, other),
                vector[:, NI : 2 * NI],
                vector[:, 2 * NI :] + jnp.where(odd, other, 0.0),
            ],
            axis=1,
        )

    def end_image(full, met, facing, at):
        left, middle, right = full[:, :NI], full[:, NI : 2 * NI], full[:, 2 * NI :]
        far = rr.at[jnp.where(odd, 1, 0)]
        outer_field = nn(jnp.where(odd, -middle, -left), far[:NI, :]) + nn(
            jnp.where(odd, right, middle), far[unknowns - NI :, :]
        )
        inside = [jnp.where(odd, facing, outer_field), jnp.where(odd, outer_field, facing)]
        met.wait_recv()
        known = jumps(inside, edge[2 * at])
        carried = split_dot(known, backward_parts, 1)
        return inside, known, carried, coarse_solve(at)

    def counted(vector):
        return jnp.concatenate([jnp.where(odd, 0.0, vector[:, :NI]), vector[:, NI:]], axis=1)

    def with_corners(inside, values):
        added = split_dot(values, corner_parts, 0)
        return [inside[k] + added[:, k * unknowns : (k + 1) * unknowns] for k in range(sub_count)]

    def column(values):
        return jnp.sum(values, axis=1, keepdims=True)

    first_fields = with_corners(local, solved)
    for k in range(sub_count):
        green[k] = first_fields[k]
    for p in range(n):
        pieces[p] = piece_part(first_fields, 0, p)
    full0 = whole(vector0, sent0, 1, extra)
    inside0, known, carried, values0 = end_image(full0, met0, facing0, 1)

    step = split_dot(values0, step_parts, 0)
    vector1 = known + step[:, : 3 * NI]
    sent1 = outer_half(outermost(vector1), 2)
    send_terms(carried + step[:, 3 * NI :], 2)
    norm_row = jnp.where(lane == sublane, column(full0 * counted(vector0)), 0.0) + jnp.where(
        lane == sublane + 8, column(full0 * counted(vector1)), 0.0
    )
    norms[0, me] = jnp.sum(norm_row, axis=0, keepdims=True)
    broadcast(norms, 0, 3)
    met1, facing1 = facing_field(vector1, 2)
    fields0 = with_corners(inside0, values0)
    for p in range(n):
        pieces[p] = pieces[p] + piece_part(fields0, 1, p)
    load_basis.wait()
    keep_split(basis_parts, basis[...])
    full1 = whole(vector1, sent1, 2)
    weighed0, weighed1 = [
        split_dot(counted(full), step_parts.at[:, :, pl.ds(0, 3 * NI)], 1) for full in (full0, full1)
    ]
    inside1, known, carried, values1 = end_image(full1, met1, facing1, 2)
    fields1 = with_corners(inside1, values1)

    all_but_one(norms, 0, wide_recv.at[3]).wait()
    totals = jnp.broadcast_to(jnp.sum(norms[0], axis=0), (8, LANES))
    norm0, curve0 = [column(jnp.where(lane == sublane + 8 * which, totals, 0.0)) for which in range(2)]
    alpha0 = norm0 / curve0
    residual = counted(full0 - alpha0 * full1)
    free = lax.rem(spot + 3, per_tile) * width + per_piece
    extra = (
        jnp.where(lane == free, column(residual * (vector0 - alpha0 * vector1)), 0.0)
        + jnp.where(
            lane == free + 1,
            column(residual * (vector1 - alpha0 * known))
            - alpha0 * column((weighed0 - alpha0 * weighed1) * values1),
            0.0,
        )
        + jnp.where(lane == free + 2, column(residual * vector1), 0.0)
    )
    for p in range(n):
        pieces[p] = pieces[p] + piece_part(fields1, 2, p) + extra
    for t in range(n):
        outgoing[t] = pieces[inverse[t]]

    def send_piece(rank):
        remote(outgoing.at[rank], incoming.at[0, me], wide_send.at[4], wide_recv.at[4], rank).start()

    others(send_piece)
    incoming[0, me] = outgoing[me]
    keep_columns(basis_across, basis[...].T)
    all_but_one(incoming, 0, wide_recv.at[4]).wait()
    gathered_sums = jnp.zeros((8, LANES), jnp.float32)
    for i in range(per_tile):
        total = incoming[0, i]
        for j in range(1, n // per_tile):
            total = total + incoming[0, j * per_tile + i]
        at = (i + 3) % per_tile * width + per_piece
        gathered_sums = jnp.where((lane >= at) & (lane < at + 3), total, gathered_sums)
    norm1, curve_rr, curve_rp = [
        column(jnp.where(lax.rem(lane, width) == per_piece + which, gathered_sums, 0.0)) for which in range(3)
    ]
    beta = norm1 / norm0
    curve1 = curve_rr + 2.0 * beta * curve_rp + beta * beta * curve0
    alpha1 = norm1 / curve1
    scale0 = alpha0 + alpha1 * (1.0 + beta)
    scale1 = -alpha1 * alpha0

    snapshot_tiles = []
    for j in range(n // per_tile):
        total = jnp.zeros((8, LANES), jnp.float32)
        for which, factor in enumerate((1.0, -scale0, -scale1)):
            tile = incoming[0, j * per_tile]
            for i in range(1, per_tile):
                block = (i + which) % per_tile
                inside = (lane >= block * width) & (lane < (block + 1) * width)
                tile = jnp.where(inside, incoming[0, j * per_tile + i], tile)
            if which:
                tile = pltpu.roll(tile, LANES - which * width, 1)
            total = total + factor * tile
        snapshot_tiles.append(total)
    snapshots = jnp.concatenate(snapshot_tiles, axis=1)
    proj_parts[seat] = split_dot(snapshots, basis_parts, 0)
    for there in seats[:-1]:
        rank = plane * inner + there
        remote(proj_parts.at[seat], proj_parts.at[seat], wide_send.at[5], wide_recv.at[5], rank).start()

    for copy in halos + coarse_near + [coarse_far] + edges:
        copy.wait_send()
    for at in range(3):
        all_but_one(gathered, at, wide_send.at[at]).wait()
    all_but_one(norms, 0, wide_send.at[3]).wait()
    all_but_one(incoming, 0, wide_send.at[4]).wait()

    for k in range(sub_count):
        carried = green[k] - scale0 * fields0[k] - scale1 * fields1[k]
        now, vel, acc = disp_now[:, k, :], vel_now[:, k, :], acc_now[:, k, :]
        accel_new = (
            (carried - now) / (newmark_beta * time_step * time_step)
            - vel / (newmark_beta * time_step)
            - (0.5 / newmark_beta - 1.0) * acc
        )
        disp_out[:, k, :] = carried
        vel_out[:, k, :] = vel + time_step * ((1.0 - newmark_gamma) * acc + newmark_gamma * accel_new)

    pltpu.make_async_copy(
        proj_parts.at[pl.ds(0, inner - 1)], proj_parts.at[pl.ds(0, inner - 1)], wide_recv.at[5]
    ).wait()
    proj_sums[plane] = jnp.sum(proj_parts[...], axis=0)
    for i in range(1, outer):
        rank = lax.rem(plane + i, outer) * inner + seat
        remote(proj_sums.at[plane], proj_sums.at[plane], wide_send.at[7], wide_recv.at[7], rank).start()
    pltpu.make_async_copy(
        proj_sums.at[pl.ds(0, outer - 1)], proj_sums.at[pl.ds(0, outer - 1)], wide_recv.at[7]
    ).wait()
    projection = jnp.sum(proj_sums[...], axis=0)
    proj_out[...] = projection
    remainder = snapshots - split_dot(projection, basis_across, 0)
    gram_row = jnp.zeros((8, LANES), jnp.float32)
    for shift in range(5):
        product = remainder * pltpu.roll(remainder, shift, 0)
        other = lax.rem(sublane + 8 - shift, 8)
        here = (lane == 8 * sublane + other) | ((lane == 8 * other + sublane) & (shift < 4))
        gram_row = jnp.where(here, column(product), gram_row)
    gram_parts[0, me] = jnp.sum(gram_row, axis=0, keepdims=True)
    broadcast(gram_parts, 0, 6)
    pltpu.make_async_copy(
        proj_parts.at[pl.ds(0, inner - 1)], proj_parts.at[pl.ds(0, inner - 1)], wide_send.at[5]
    ).wait()
    pltpu.make_async_copy(
        proj_sums.at[pl.ds(0, outer - 1)], proj_sums.at[pl.ds(0, outer - 1)], wide_send.at[7]
    ).wait()
    all_but_one(gram_parts, 0, wide_recv.at[6]).wait()
    gram_row = jnp.broadcast_to(jnp.sum(gram_parts[0], axis=0), (8, LANES))
    entry = {
        (i, j): jnp.broadcast_to(gram_row[:, 8 * i + j : 8 * i + j + 1], (8, LANES)) for i in range(8) for j in range(i + 1)
    }
    row_at = lax.broadcasted_iota(jnp.int32, remainder.shape, 0)
    factor = jnp.zeros((8, LANES), jnp.float32)
    for j in range(8):
        inverse_root = lax.rsqrt(entry[j, j])
        lower = {i: entry[i, j] * inverse_root for i in range(j, 8)}
        below = jnp.zeros((8, LANES), jnp.float32)
        for i in range(j, 8):
            factor = jnp.where((sublane == j) & (lane == i), lower[i], factor)
            for k in range(j + 1, i + 1):
                entry[i, k] = entry[i, k] - lower[i] * lower[k]
            if i > j:
                below = jnp.where(sublane == i, lower[i], below)
        pivot_rows = remainder[j : j + 1, :] * inverse_root[0:1, 0:1]
        remainder = jnp.where(row_at == j, pivot_rows, remainder - below[:, 0:1] * pivot_rows)
    scale_rows = math.sqrt(snapshots.shape[1] * n)
    r_out[...] = factor[:, :8] * (1.0 / scale_rows)
    cols_out[...] = remainder * scale_rows

    all_but_one(gram_parts, 0, wide_send.at[6]).wait()


def solution(mesh):
    groups = mesh.shape["grp"]
    n = mesh.shape["sub"] * groups
    inner = math.gcd(n, 8)

    def shards(
        rr_inverse,
        corner_modes,
        coarse_inverse,
        inertia,
        disp_now,
        vel_now,
        acc_now,
        load_next,
        basis_rows,
        piece_owner,
    ):
        case_count, sub_count, unknowns = disp_now.shape
        rank = basis_rows.shape[1]
        local_rows = basis_rows.shape[0]
        width = (sub_count + 2) * NC
        f32 = jnp.float32
        vmem = pl.BlockSpec(memory_space=pltpu.VMEM)
        anywhere = pl.BlockSpec(memory_space=pl.ANY)
        results = (
            jax.ShapeDtypeStruct(disp_now.shape, f32),
            jax.ShapeDtypeStruct(disp_now.shape, f32),
            jax.ShapeDtypeStruct((case_count, rank), f32),
            jax.ShapeDtypeStruct((case_count, case_count), f32),
            jax.ShapeDtypeStruct((case_count, local_rows), f32),
        )
        kept = tuple(pltpu.VMEM(result.shape, f32) for result in results)
        computed = pl.pallas_call(
            functools.partial(kernel, n, groups, inner),
            out_shape=kept,
            in_specs=[anywhere] * 10,
            out_specs=(vmem,) * 5,
            scratch_shapes=[
                pltpu.SMEM(piece_owner.shape, jnp.int32),
                pltpu.SMEM(piece_owner.shape, jnp.int32),
                pltpu.VMEM(inertia.shape, f32),
                pltpu.VMEM(disp_now.shape, f32),
                pltpu.VMEM(vel_now.shape, f32),
                pltpu.VMEM(acc_now.shape, f32),
                pltpu.VMEM(load_next.shape, f32),
                pltpu.VMEM((2, coarse_inverse.shape[1], width), jnp.bfloat16),
                pltpu.VMEM((2, width, (sub_count + 4) * NI), jnp.bfloat16),
                pltpu.VMEM((2, width, (sub_count + 1) * NI + width), jnp.bfloat16),
                pltpu.VMEM((2, width, (sub_count + 2) * NI), jnp.bfloat16),
                pltpu.VMEM((2, width, (sub_count + 1) * NI), jnp.bfloat16),
                pltpu.VMEM((2, width, sub_count * unknowns), jnp.bfloat16),
                pltpu.VMEM((2,) + basis_rows.shape, jnp.bfloat16),
                pltpu.VMEM((2,) + basis_rows.shape[::-1], jnp.bfloat16),
                pltpu.VMEM(rr_inverse.shape, f32),
                pltpu.VMEM(corner_modes.shape, f32),
                pltpu.VMEM((width + NC, coarse_inverse.shape[1]), f32),
                pltpu.VMEM(basis_rows.shape, f32),
                pltpu.VMEM((3, 2 * NC, NI), f32),
                pltpu.VMEM((2 * NC, NI), f32),
                pltpu.VMEM((width, sub_count * unknowns), f32),
                pltpu.VMEM((width, (sub_count + 1) * NI), f32),
                pltpu.VMEM((width, (sub_count + 1) * NI), f32),
                pltpu.VMEM((3, n, case_count, width), f32),
                pltpu.VMEM((6, case_count, NI), f32),
                pltpu.VMEM((6, case_count, NI), f32),
                pltpu.VMEM((1, n, 1, LANES), f32),
                pltpu.VMEM((n, case_count, LANES), f32),
                pltpu.VMEM((n, case_count, LANES), f32),
                pltpu.VMEM((1, n, case_count, LANES), f32),
                pltpu.VMEM((inner, case_count, rank), f32),
                pltpu.VMEM((n // inner, case_count, rank), f32),
                pltpu.VMEM((1, n, 1, LANES), f32),
                pltpu.VMEM((sub_count, case_count, unknowns), f32),
                pltpu.SemaphoreType.DMA((10,)),
                pltpu.SemaphoreType.DMA((7,)),
                pltpu.SemaphoreType.DMA((7,)),
                pltpu.SemaphoreType.DMA((8,)),
                pltpu.SemaphoreType.DMA((8,)),
                pltpu.SemaphoreType.DMA((6,)),
                pltpu.SemaphoreType.DMA((6,)),
            ],
            compiler_params=pltpu.CompilerParams(collective_id=0, has_side_effects=True),
        )(
            piece_owner,
            rr_inverse,
            corner_modes,
            coarse_inverse,
            basis_rows,
            inertia,
            disp_now,
            vel_now,
            acc_now,
            load_next,
        )
        disp, vel, proj, r_factor, columns = pl.pallas_call(
            hand_over,
            out_shape=results,
            in_specs=[vmem] * 5,
            out_specs=(vmem,) * 5,
            compiler_params=pltpu.CompilerParams(vmem_limit_bytes=4 * 1024 * 1024),
        )(*computed)
        return disp, vel, proj.T, r_factor, columns

    return jax.shard_map(
        shards,
        mesh=mesh,
        in_specs=(
            P(("sub", "grp"), None, None),
            P(("sub", "grp"), None, None),
            P(("sub", "grp"), None),
            P(("sub", "grp"), None),
            P(None, ("sub", "grp"), None),
            P(None, ("sub", "grp"), None),
            P(None, ("sub", "grp"), None),
            P(None, ("sub", "grp"), None),
            P(("sub", "grp"), None),
            P(),
        ),
        out_specs=(
            P(None, ("sub", "grp"), None),
            P(None, ("sub", "grp"), None),
            P(),
            P(),
            P(None, ("sub", "grp")),
        ),
        check_vma=False,
    )
```
